768 devices in a mesh: curve: 96 (over y, z), seg: 8 (over x, core).
Axes of the slice: x: 4, y: 8, z: 12, core: 2. Of those that a mesh axis runs over, the one named last changes fastest.
Arguments:
- solution: bfloat16 [393216, 128], P(('curve', 'seg')), may hold values from -6 to 6
- viscosity: float32 [3145728], P(('curve', 'seg')), may hold values from 0.1 to 10
- slot_index: int32 [3145728, 4], P(('curve', 'seg')), may hold values from 0 to 1279, as said below
- slot_weight: int32 [3145728, 4], P(('curve', 'seg')), may hold values from -1 to 8, as said below
- mirror_rows: int32 [768, 4, 192], P(('curve', 'seg')), may hold values from 0 to 511
- ghost_live: int32 [768, 4], P(('curve', 'seg')), may hold values from 0 to 192, as said below
- cell_count: int32 [768], P(('curve', 'seg')), may hold values from 512 to 4096, as said below
- viscous_block: bfloat16 [128, 128], replicated, may hold values from -0.5 to 0.5
- pressure_block: bfloat16 [128, 128], replicated, may hold values from -0.5 to 0.5
Outputs:
- residual: float32 [393216, 128], P(('curve', 'seg'))
The draws below stay inside these ranges and needn't reach their ends.
Inputs may be any that keep to these rules, and one draw needn't show every extreme that they name: `slot_index`: column 0 of each element is one of its device's owned blocks; other columns point to owned blocks or to ghost entries; ghost entries past a list's live count read zeros. `slot_weight`: each entry is one of -1, 3, 6, 8; column 0 is 8. `ghost_live`: some list is full in every draw. `cell_count`: some device is full in every draw; loads are skewed.
All inputs are finite; a program needn't handle non-finite values.
Results may differ from the reference program's by a relative error of at most 0.0035.
Values may be sent and summed in bfloat16 or wider, within the bound.
A program may use at most 32 MiB of HBM per device.

```python
import math
import jax
import jax.numpy as jnp
from jax import lax

BLOCK = 128
SLOTS = 4
REACH = 2
NB_DEV = 512
E_DEV = 4096
GHOST = 192
NOFF = 4
BLOCKS = 393216
ELEMS = 3145728
N_CURVE = 96
N_SEG = 8


def draw_slot_index(key, part):
    own_key = jax.random.fold_in(key, 11)
    pick_key = jax.random.fold_in(key, 12)
    ghost_key = jax.random.fold_in(key, 13)
    owned = jax.random.randint(own_key, (ELEMS, SLOTS), 0, NB_DEV)
    ghosts = NB_DEV + jax.random.randint(ghost_key, (ELEMS, SLOTS), 0, 2 * REACH * GHOST)
    picked = jax.random.randint(pick_key, (ELEMS, SLOTS), 0, 10) < 3
    picked = picked.at[:, 0].set(False)
    return jnp.where(picked, ghosts, owned).astype(jnp.int32)


def draw_slot_weight(key, part):
    table = jnp.array([-1, 3, 6, 8], dtype=jnp.int32)
    picks = jax.random.randint(jax.random.fold_in(key, 21), (ELEMS, SLOTS), 0, 4)
    codes = table[picks]
    return codes.at[:, 0].set(8).astype(jnp.int32)


def draw_ghost_live(key, part):
    devices_all = N_CURVE * N_SEG
    counts = jax.random.randint(jax.random.fold_in(key, 31), (devices_all, 2 * REACH), 0, GHOST + 1)
    device = jax.random.randint(jax.random.fold_in(key, 32), (), 0, devices_all)
    region = jax.random.randint(jax.random.fold_in(key, 33), (), 0, 2 * REACH)
    return counts.at[device, region].set(GHOST).astype(jnp.int32)


def draw_cell_count(key, part):
    devices_all = N_CURVE * N_SEG
    full = jax.random.randint(jax.random.fold_in(key, 41), (devices_all,), 0, 8) == 0
    shifts = jax.random.randint(jax.random.fold_in(key, 42), (devices_all,), 2, 4)
    counts = jnp.where(full, E_DEV, jnp.right_shift(jnp.full((devices_all,), E_DEV, jnp.int32), shifts))
    device = jax.random.randint(jax.random.fold_in(key, 43), (), 0, devices_all)
    return counts.at[device].set(E_DEV).astype(jnp.int32)


def set_ends(drawn, key, smallest, largest):
    longest = drawn.shape.index(max(drawn.shape))
    spots = []
    for shift in (0, 1):
        where = [jax.random.randint(jax.random.fold_in(key, axis), (), 0, length) for axis, length in enumerate(drawn.shape)]
        where[longest] = (where[longest] + shift) % drawn.shape[longest]
        spots.append(tuple(where))
    return drawn.at[spots[0]].set(smallest).at[spots[1]].set(largest)


def level_of(stream_key, extent, cuts, smallest, high):
    factor_of = 1.0
    for dim, shards_of in cuts:
        heights = jax.random.uniform(jax.random.fold_in(jax.random.fold_in(stream_key, 6), dim), (shards_of,), jnp.float32, smallest / len(cuts), high / len(cuts))
        factor_of = factor_of * jnp.repeat(jnp.exp(heights), extent[dim] // shards_of).reshape((-1,) + (1,) * (len(extent) - 1 - dim))
    return factor_of


def centred(stream_key, shape, scale, most, split=(), held_as=jnp.bfloat16):
    entries = scale * jax.random.normal(stream_key, shape, jnp.float32)
    if split:
        entries = entries * level_of(stream_key, shape, split, -0.22, 0.18)
    return jnp.clip(entries, -most, most).astype(held_as)


def setup_inputs(seed: int = 0) -> dict:
    keys = jax.random.split(jax.random.key(seed), 10)
    return {
        "solution": centred(keys[0], (BLOCKS, BLOCK), 1.0, 6.0, ((0, 768),)),
        "viscosity": jnp.clip(jnp.exp(math.log(10.0) - 4.6051702 * jax.random.uniform(keys[1], (ELEMS,), jnp.float32) ** level_of(keys[1], (ELEMS,), ((0, 768),), -0.2, 0.2)), 0.1, 10.0),
        "slot_index": draw_slot_index(jax.random.fold_in(keys[9], 71), 0),
        "slot_weight": draw_slot_weight(jax.random.fold_in(keys[9], 71), 0),
        "mirror_rows": set_ends(jax.random.randint(keys[4], (N_CURVE * N_SEG, NOFF, GHOST), 0, NB_DEV), jax.random.fold_in(keys[4], 1), 0, NB_DEV - 1).astype(jnp.int32),
        "ghost_live": draw_ghost_live(jax.random.fold_in(keys[9], 71), 0),
        "cell_count": draw_cell_count(jax.random.fold_in(keys[9], 71), 0),
        "viscous_block": centred(keys[7], (BLOCK, BLOCK), BLOCK ** -0.5, 0.5),
        "pressure_block": centred(keys[8], (BLOCK, BLOCK), BLOCK ** -0.5, 0.5),
    }


def shift_list(region_count):
    return [(region // 2 + 1) * (1 if region % 2 == 0 else -1) for region in range(region_count)]


def reference(solution, viscosity, slot_index, slot_weight, mirror_rows, ghost_live, cell_count, viscous_block, pressure_block):
    devices_all = N_CURVE * N_SEG
    offsets = shift_list(2 * REACH)
    owned_all = solution.reshape(devices_all, NB_DEV, BLOCK)
    ghost_pos = jnp.arange(GHOST, dtype=jnp.int32)
    elem_pos = jnp.arange(E_DEV, dtype=jnp.int32)

    def device_part(device):
        pieces = [owned_all[device]]
        for region, offset in enumerate(offsets):
            source = device - offset
            valid = (source >= 0) & (source < devices_all)
            sender = jnp.clip(source, 0, devices_all - 1).astype(jnp.int32)
            rows = owned_all[sender][mirror_rows[sender, region]]
            keep = valid & (ghost_pos < ghost_live[sender, region])
            pieces.append(jnp.where(keep[:, None], rows, jnp.zeros_like(rows)))
        extended = jnp.concatenate(pieces, axis=0)
        start = (device * E_DEV).astype(jnp.int32)
        indices = lax.dynamic_slice_in_dim(slot_index, start, E_DEV, 0)
        codes = lax.dynamic_slice_in_dim(slot_weight, start, E_DEV, 0)
        local_visc = lax.dynamic_slice_in_dim(viscosity, start, E_DEV, 0)
        live = (elem_pos < cell_count[device]).astype(jnp.float32)
        weights = codes.astype(jnp.float32) / 8.0 * live[:, None]
        element_in = jnp.zeros((E_DEV, BLOCK), jnp.float32)
        for slot_pos in range(SLOTS):
            element_in = element_in + weights[:, slot_pos, None] * extended[indices[:, slot_pos]].astype(jnp.float32)
        element_in = element_in.astype(jnp.bfloat16)
        element_out = local_visc[:, None] * jnp.dot(element_in, viscous_block, preferred_element_type=jnp.float32)
        element_out = element_out + jnp.dot(element_in, pressure_block, preferred_element_type=jnp.float32)
        partial_value = jnp.zeros((NB_DEV + 2 * REACH * GHOST, BLOCK), jnp.float32)
        for slot_pos in range(SLOTS):
            partial_value = partial_value.at[indices[:, slot_pos]].add(weights[:, slot_pos, None] * element_out)
        return partial_value[:NB_DEV], partial_value[NB_DEV:].reshape(2 * REACH, GHOST, BLOCK)

    owned_part, ghost_part = lax.map(device_part, jnp.arange(devices_all, dtype=jnp.int32))

    def finish(device):
        total = owned_part[device]
        for region, offset in enumerate(offsets):
            target = device + offset
            valid = (target >= 0) & (target < devices_all)
            holder = jnp.clip(target, 0, devices_all - 1).astype(jnp.int32)
            piece = ghost_part[holder, region]
            keep = valid & (ghost_pos < ghost_live[device, region])
            total = total.at[mirror_rows[device, region]].add(jnp.where(keep[:, None], piece, jnp.zeros_like(piece)))
        return total

    residual = lax.map(finish, jnp.arange(devices_all, dtype=jnp.int32))
    return residual.reshape(NB_DEV * devices_all, BLOCK)
```

```python
import functools

import jax
import jax.numpy as jnp
from jax import lax
from jax.experimental import pallas as pl
from jax.experimental.pallas import tpu as pltpu
from jax.sharding import PartitionSpec as P

LANES = 128
MESH = pl.DeviceIdType.MESH


def shift_list(region_count):
    return [(region // 2 + 1) * (1 if region % 2 == 0 else -1) for region in range(region_count)]


def contract(lhs, rhs, lhs_dim, rhs_dim):
    return lax.dot_general(
        lhs, rhs, (((lhs_dim,), (rhs_dim,)), ((), ())), preferred_element_type=jnp.float32
    )


def operator_kernel(
    n_curve,
    n_seg,
    live_ref,
    count_ref,
    solution_ref,
    visc_ref,
    index_ref,
    weight_ref,
    mirror_ref,
    viscous_ref,
    pressure_ref,
    out_ref,
    column_ids,
    table,
    mirror_table,
    dofs_t,
    gathered,
    element_out,
    outgoing,
    ghosts,
    back_out,
    back_in,
    send_sem,
    recv_sem,
    back_send_sem,
    back_recv_sem,
):
    owned = solution_ref.shape[0]
    width = solution_ref.shape[1]
    regions, ghost_rows = mirror_ref.shape
    slots, elems = index_ref.shape
    columns = table.shape[0]
    ghost_total = columns - owned
    pad_rows = mirror_table.shape[1] // regions
    devices = n_curve * n_seg
    offsets = shift_list(regions)
    me = lax.axis_index("curve") * n_seg + lax.axis_index("seg")

    def place(device):
        return (device // n_seg, lax.rem(device, n_seg))

    def exists(device):
        return jnp.logical_and(device >= 0, device < devices)

    barrier = pltpu.get_barrier_semaphore()
    for offset in offsets:
        @pl.when(exists(me + offset))
        def _():
            pl.semaphore_signal(barrier, inc=1, device_id=place(me + offset), device_id_type=MESH)

    rows = lax.broadcasted_iota(jnp.int32, (owned, ghost_rows), 0)
    entry = lax.broadcasted_iota(jnp.int32, (1, ghost_rows), 1)
    mirror_table[...] = jnp.zeros_like(mirror_table)
    for region in range(regions):
        picks = jnp.where(entry < live_ref[0, region], mirror_ref[region : region + 1, :], -1)
        hit = (rows == picks).astype(jnp.float32).astype(jnp.bfloat16)
        mirror_table[:, region * pad_rows : region * pad_rows + ghost_rows] = hit
    dofs_t[:, :owned] = solution_ref[...].astype(jnp.float32).T.astype(jnp.bfloat16)
    listed = contract(dofs_t[:, :owned], mirror_table[...], 1, 0)
    outgoing[...] = listed.T.astype(jnp.bfloat16)

    peers = sum(exists(me + offset).astype(jnp.int32) for offset in offsets)
    pl.semaphore_wait(barrier, peers)

    def ghost_copy(region):
        return pltpu.make_async_remote_copy(
            src_ref=outgoing.at[pl.ds(region * pad_rows, ghost_rows)],
            dst_ref=ghosts.at[pl.ds(region * ghost_rows, ghost_rows)],
            send_sem=send_sem.at[region],
            recv_sem=recv_sem.at[region],
            device_id=place(me + offsets[region]),
            device_id_type=MESH,
        )

    for region in range(regions):
        @pl.when(exists(me + offsets[region]))
        def _():
            ghost_copy(region).start()

        @pl.when(jnp.logical_not(exists(me - offsets[region])))
        def _():
            ghosts[region * ghost_rows : (region + 1) * ghost_rows] = jnp.zeros(
                (ghost_rows, width), jnp.bfloat16
            )

    sub = 16
    column_ids[...] = lax.broadcasted_iota(jnp.int32, column_ids.shape, 0).astype(jnp.int16)
    count = count_ref[0]
    chunk = min(512, elems)

    def build(step, carry):
        for group in range(chunk // LANES):
            start = pl.multiple_of(step * chunk + group * LANES, LANES)
            lanes = pl.ds(start, LANES)
            live = (lax.broadcasted_iota(jnp.int32, (1, LANES), 1) + start) < count
            index = [index_ref[slot : slot + 1, lanes] for slot in range(slots)]
            raw = [
                jnp.where(live, weight_ref[slot : slot + 1, lanes].astype(jnp.float32) * 0.125, 0.0)
                for slot in range(slots)
            ]
            merged = []
            for slot in range(slots):
                value = raw[slot]
                for other in range(slot):
                    value = value + jnp.where(index[other] == index[slot], raw[other], 0.0)
                merged.append(value)
            ids = [jnp.broadcast_to(i, (sub, LANES)).astype(jnp.int16) for i in index]
            wts = [jnp.broadcast_to(v, (sub, LANES)).astype(jnp.bfloat16) for v in merged]
            for block in range(columns // sub):
                here = slice(block * sub, (block + 1) * sub)
                ident = column_ids[here, :]
                value = jnp.zeros((sub, LANES), jnp.bfloat16)
                first = 0 if block * sub < owned else 1
                for slot in range(first, slots):
                    value = jnp.where(ident == ids[slot], wts[slot], value)
                table[here, lanes] = value
        lanes = pl.ds(pl.multiple_of(step * chunk, chunk), chunk)
        gathered[:, lanes] = contract(dofs_t[:, :owned], table[:owned, lanes], 1, 0)
        return carry

    lax.fori_loop(0, elems // chunk, build, 0)

    for region in range(regions):
        @pl.when(exists(me - offsets[region]))
        def _():
            ghost_copy(region).wait_recv()

    dofs_t[:, owned:] = ghosts[...].astype(jnp.float32).T.astype(jnp.bfloat16)
    viscous = viscous_ref[...].astype(jnp.float32).T.astype(jnp.bfloat16)
    pressure = pressure_ref[...].astype(jnp.float32).T.astype(jnp.bfloat16)

    def apply(step, carry):
        lanes = pl.ds(pl.multiple_of(step * chunk, chunk), chunk)
        total = gathered[:, lanes] + contract(dofs_t[:, owned:], table[owned:, lanes], 1, 0)
        element_in = total.astype(jnp.bfloat16)
        result = contract(viscous, element_in, 1, 0) * visc_ref[:, lanes]
        result = result + contract(pressure, element_in, 1, 0)
        element_out[:, lanes] = result.astype(jnp.bfloat16)
        return carry

    lax.fori_loop(0, elems // chunk, apply, 0)

    def back_copy(region):
        return pltpu.make_async_remote_copy(
            src_ref=back_out.at[pl.ds(region * ghost_rows, ghost_rows)],
            dst_ref=back_in.at[pl.ds(region * pad_rows, ghost_rows)],
            send_sem=back_send_sem.at[region],
            recv_sem=back_recv_sem.at[region],
            device_id=place(me - offsets[region]),
            device_id_type=MESH,
        )

    for region in range(regions):
        back_in[region * pad_rows + ghost_rows : (region + 1) * pad_rows] = jnp.zeros(
            (pad_rows - ghost_rows, width), jnp.bfloat16
        )

        @pl.when(jnp.logical_not(exists(me + offsets[region])))
        def _():
            back_in[region * pad_rows : region * pad_rows + ghost_rows] = jnp.zeros(
                (ghost_rows, width), jnp.bfloat16
            )

    ghost_part = contract(element_out[...], table[owned:], 1, 1)
    back_out[...] = ghost_part.T.astype(jnp.bfloat16)
    for region in range(regions):
        @pl.when(exists(me - offsets[region]))
        def _():
            back_copy(region).start()

    own_part = contract(element_out[...], table[:owned], 1, 1)
    out_ref[...] = own_part.T

    for region in range(regions):
        @pl.when(exists(me + offsets[region]))
        def _():
            back_copy(region).wait_recv()

    out_ref[...] += contract(mirror_table[...], back_in[...], 1, 0)

    for region in range(regions):
        @pl.when(exists(me + offsets[region]))
        def _():
            ghost_copy(region).wait_send()

        @pl.when(exists(me - offsets[region]))
        def _():
            back_copy(region).wait_send()


def per_device(
    n_curve,
    n_seg,
    solution,
    viscosity,
    slot_index,
    slot_weight,
    mirror_rows,
    ghost_live,
    cell_count,
    viscous_block,
    pressure_block,
):
    owned, width = solution.shape
    elems, slots = slot_index.shape
    regions, ghost_rows = mirror_rows.shape[1:]
    pad_rows = -(-ghost_rows // LANES) * LANES
    columns = owned + regions * ghost_rows
    vmem = pl.BlockSpec(memory_space=pltpu.VMEM)
    smem = pl.BlockSpec(memory_space=pltpu.SMEM)
    bf16 = jnp.bfloat16
    return pl.pallas_call(
        functools.partial(operator_kernel, n_curve, n_seg),
        out_shape=jax.ShapeDtypeStruct((owned, width), jnp.float32),
        in_specs=[smem, smem] + [vmem] * 7,
        out_specs=vmem,
        scratch_shapes=[
            pltpu.VMEM((columns, LANES), jnp.int16),
            pltpu.VMEM((columns, elems), bf16),
            pltpu.VMEM((owned, regions * pad_rows), bf16),
            pltpu.VMEM((width, columns), bf16),
            pltpu.VMEM((width, elems), jnp.float32),
            pltpu.VMEM((width, elems), bf16),
            pltpu.VMEM((regions * pad_rows, width), bf16),
            pltpu.VMEM((regions * ghost_rows, width), bf16),
            pltpu.VMEM((regions * ghost_rows, width), bf16),
            pltpu.VMEM((regions * pad_rows, width), bf16),
            pltpu.SemaphoreType.DMA((regions,)),
            pltpu.SemaphoreType.DMA((regions,)),
            pltpu.SemaphoreType.DMA((regions,)),
            pltpu.SemaphoreType.DMA((regions,)),
        ],
        compiler_params=pltpu.CompilerParams(
            collective_id=0, has_side_effects=True, vmem_limit_bytes=48 * 1024 * 1024
        ),
    )(
        ghost_live,
        cell_count,
        solution,
        viscosity.reshape(1, elems),
        slot_index.T,
        slot_weight.T,
        mirror_rows.reshape(regions, ghost_rows),
        viscous_block,
        pressure_block,
    )


def solution(mesh):
    return jax.shard_map(
        functools.partial(per_device, mesh.shape["curve"], mesh.shape["seg"]),
        mesh=mesh,
        in_specs=(
            P(("curve", "seg"), None),
            P(("curve", "seg")),
            P(("curve", "seg"), None),
            P(("curve", "seg"), None),
            P(("curve", "seg"), None, None),
            P(("curve", "seg"), None),
            P(("curve", "seg")),
            P(),
            P(),
        ),
        out_specs=P(("curve", "seg"), None),
        check_vma=False,
    )
```

```python
import functools

import jax
import jax.numpy as jnp
from jax import lax
from jax.experimental import pallas as pl
from jax.experimental.pallas import tpu as pltpu
from jax.sharding import PartitionSpec as P

LANES = 128
MESH = pl.DeviceIdType.MESH


def shift_list(region_count):
    return [(region // 2 + 1) * (1 if region % 2 == 0 else -1) for region in range(region_count)]


def contract(lhs, rhs, lhs_dim, rhs_dim):
    return lax.dot_general(
        lhs, rhs, (((lhs_dim,), (rhs_dim,)), ((), ())), preferred_element_type=jnp.float32
    )


def operator_kernel(
    n_curve,
    n_seg,
    count_ref,
    solution_hbm,
    visc_hbm,
    index_hbm,
    weight_hbm,
    mirror_hbm,
    live_hbm,
    viscous_hbm,
    pressure_hbm,
    out_ref,
    solution_ref,
    visc_ref,
    index_ref,
    weight_ref,
    mirror_ref,
    live_ref,
    viscous_ref,
    pressure_ref,
    table,
    mirror_table,
    dofs_t,
    gathered,
    element_out,
    outgoing,
    ghosts,
    back_out,
    back_in,
    load_sem,
    send_sem,
    recv_sem,
    back_send_sem,
    back_recv_sem,
):
    owned, width = solution_ref.shape
    regions, ghost_rows = mirror_ref.shape
    slots, elems = index_ref.shape
    groups, columns, lanes_of = table.shape
    pad_rows = mirror_table.shape[1] // regions
    devices = n_curve * n_seg
    offsets = shift_list(regions)
    order = [k for k in range(regions) if offsets[k] > 0]
    half = len(order)
    order = order + [k for k in range(regions) if offsets[k] < 0]
    place_of = {region: pos for pos, region in enumerate(order)}
    split = half * ghost_rows
    me = lax.axis_index("curve") * n_seg + lax.axis_index("seg")

    def place(device):
        return (device // n_seg, lax.rem(device, n_seg))

    def exists(device):
        return jnp.logical_and(device >= 0, device < devices)

    barrier = pltpu.get_barrier_semaphore()
    for offset in offsets:
        @pl.when(exists(me + offset))
        def _():
            pl.semaphore_signal(barrier, inc=1, device_id=place(me + offset), device_id_type=MESH)

    pairs = [
        (mirror_hbm, mirror_ref),
        (live_hbm, live_ref),
        (solution_hbm, solution_ref),
        (index_hbm, index_ref),
        (weight_hbm, weight_ref),
        (visc_hbm, visc_ref),
        (viscous_hbm, viscous_ref),
        (pressure_hbm, pressure_ref),
    ]
    loads = [
        pltpu.make_async_copy(source, target, load_sem.at[pos])
        for pos, (source, target) in enumerate(pairs)
    ]
    for load in loads:
        load.start()

    sub = 16
    row16 = lax.broadcasted_iota(jnp.int32, (sub, lanes_of), 0).astype(jnp.int16)
    one = jnp.ones((sub, lanes_of), jnp.bfloat16)
    zero = jnp.zeros((sub, lanes_of), jnp.bfloat16)

    for load in loads[:3]:
        load.wait()
    for pos, region in enumerate(order):
        for part in range(pad_rows // LANES):
            first = part * LANES
            size = min(LANES, ghost_rows - first)
            entry = lax.broadcasted_iota(jnp.int32, (1, LANES), 1) + first
            picks = mirror_ref[region : region + 1, first : first + size]
            if size < LANES:
                picks = jnp.concatenate([picks, jnp.full((1, LANES - size), -1, jnp.int32)], axis=1)
            limit = jnp.minimum(live_ref[0:1, region : region + 1], ghost_rows)
            picks = jnp.where(entry < limit, picks, -1)
            picks = jnp.broadcast_to(picks, (sub, LANES)).astype(jnp.int16) - row16
            for block in range(owned // sub):
                hit = jnp.where(picks == jnp.int16(block * sub), one, zero)
                start = pos * pad_rows + first
                mirror_table[block * sub : (block + 1) * sub, start : start + LANES] = hit
    dofs_t[:, :owned] = solution_ref[...].astype(jnp.float32).T.astype(jnp.bfloat16)
    listed = contract(dofs_t[:, :owned], mirror_table[...], 1, 0)
    outgoing[...] = listed.T.astype(jnp.bfloat16)

    peers = sum(exists(me + offset).astype(jnp.int32) for offset in offsets)
    pl.semaphore_wait(barrier, peers)

    def ghost_copy(region):
        pos = place_of[region]
        return pltpu.make_async_remote_copy(
            src_ref=outgoing.at[pl.ds(pos * pad_rows, ghost_rows)],
            dst_ref=ghosts.at[pl.ds(pos * ghost_rows, ghost_rows)],
            send_sem=send_sem.at[region],
            recv_sem=recv_sem.at[region],
            device_id=place(me + offsets[region]),
            device_id_type=MESH,
        )

    for region in order:
        @pl.when(exists(me + offsets[region]))
        def _():
            ghost_copy(region).start()

    for pos, region in enumerate(order):
        @pl.when(jnp.logical_not(exists(me - offsets[region])))
        def _():
            ghosts[pos * ghost_rows : (pos + 1) * ghost_rows] = jnp.zeros(
                (ghost_rows, width), jnp.bfloat16
            )

        back_in[pos * pad_rows + ghost_rows : (pos + 1) * pad_rows] = jnp.zeros(
            (pad_rows - ghost_rows, width), jnp.bfloat16
        )

        @pl.when(jnp.logical_not(exists(me + offsets[region])))
        def _():
            back_in[pos * pad_rows : pos * pad_rows + ghost_rows] = jnp.zeros(
                (ghost_rows, width), jnp.bfloat16
            )

    for load in loads[3:5]:
        load.wait()
    per_step = min(4, groups)
    chunk = per_step * lanes_of
    count = count_ref[0]

    def moved(index):
        result = index
        for k in range(regions):
            shift = (place_of[k] - k) * ghost_rows
            if shift:
                low = owned + k * ghost_rows
                inside = jnp.logical_and(index >= low, index < low + ghost_rows)
                result = jnp.where(inside, index + shift, result)
        return result

    def build(step, carry):
        for inner in range(per_step):
            group = step * per_step + inner
            start = pl.multiple_of(group * lanes_of, lanes_of)
            lanes = pl.ds(start, lanes_of)
            live = (lax.broadcasted_iota(jnp.int32, (1, lanes_of), 1) + start) < count
            index = [moved(index_ref[slot : slot + 1, lanes]) for slot in range(slots)]
            raw = [
                jnp.where(live, weight_ref[slot : slot + 1, lanes].astype(jnp.float32) * 0.125, 0.0)
                for slot in range(slots)
            ]
            merged = []
            for slot in range(slots):
                value = raw[slot]
                for other in range(slot):
                    value = value + jnp.where(index[other] == index[slot], raw[other], 0.0)
                merged.append(value)
            shape = (sub, lanes_of)
            ids = [jnp.broadcast_to(i, shape).astype(jnp.int16) - row16 for i in index]
            wts = [jnp.broadcast_to(v, shape).astype(jnp.bfloat16) for v in merged]
            for block in range(columns // sub):
                value = zero
                for slot in range(0 if block * sub < owned else 1, slots):
                    value = jnp.where(ids[slot] == jnp.int16(block * sub), wts[slot], value)
                table[group, block * sub : (block + 1) * sub, :] = value
        gathered[:, step_lanes(step)] = contract(
            dofs_t[:, :owned], rows_of(step, 0, owned), 1, 0
        )
        return carry

    def step_lanes(step):
        return pl.ds(pl.multiple_of(step * chunk, chunk), chunk)

    def rows_of(step, low, high):
        return jnp.concatenate(
            [table[step * per_step + inner, low:high, :] for inner in range(per_step)], axis=1
        )

    steps = groups // per_step
    lax.fori_loop(0, steps, build, 0)

    def receive(chosen):
        for region in chosen:
            @pl.when(exists(me - offsets[region]))
            def _():
                ghost_copy(region).wait_recv()

    receive(order[:half])
    middle = owned + split
    dofs_t[:, owned:middle] = ghosts[:split].astype(jnp.float32).T.astype(jnp.bfloat16)

    def lower_part(step, carry):
        gathered[:, step_lanes(step)] += contract(
            dofs_t[:, owned:middle], rows_of(step, owned, middle), 1, 0
        )
        return carry

    lax.fori_loop(0, steps, lower_part, 0)
    for load in loads[5:]:
        load.wait()
    viscous = viscous_ref[...].astype(jnp.float32).T.astype(jnp.bfloat16)
    pressure = pressure_ref[...].astype(jnp.float32).T.astype(jnp.bfloat16)

    receive(order[half:])
    dofs_t[:, middle:] = ghosts[split:].astype(jnp.float32).T.astype(jnp.bfloat16)

    def apply(step, carry):
        lanes = step_lanes(step)
        total = gathered[:, lanes] + contract(
            dofs_t[:, middle:], rows_of(step, middle, columns), 1, 0
        )
        element_in = total.astype(jnp.bfloat16)
        result = contract(viscous, element_in, 1, 0) * visc_ref[:, lanes]
        result = result + contract(pressure, element_in, 1, 0)
        element_out[:, lanes] = result.astype(jnp.bfloat16)
        return carry

    lax.fori_loop(0, steps, apply, 0)

    def back_copy(region):
        pos = place_of[region]
        return pltpu.make_async_remote_copy(
            src_ref=back_out.at[pl.ds(pos * ghost_rows, ghost_rows)],
            dst_ref=back_in.at[pl.ds(pos * pad_rows, ghost_rows)],
            send_sem=back_send_sem.at[region],
            recv_sem=back_recv_sem.at[region],
            device_id=place(me - offsets[region]),
            device_id_type=MESH,
        )

    def scatter(low, high):
        rows = jnp.concatenate([table[group, low:high, :] for group in range(groups)], axis=1)
        return contract(element_out[...], rows, 1, 1).T

    back_out[split:] = scatter(middle, columns).astype(jnp.bfloat16)
    for region in order[half:]:
        @pl.when(exists(me - offsets[region]))
        def _():
            back_copy(region).start()

    back_out[:split] = scatter(owned, middle).astype(jnp.bfloat16)
    for region in order[:half]:
        @pl.when(exists(me - offsets[region]))
        def _():
            back_copy(region).start()

    out_ref[...] = scatter(0, owned)

    for chosen, low in ((order[:half], 0), (order[half:], half * pad_rows)):
        for region in chosen:
            @pl.when(exists(me + offsets[region]))
            def _():
                back_copy(region).wait_recv()

        high = low + half * pad_rows
        out_ref[...] += contract(mirror_table[:, low:high], back_in[low:high], 1, 0)

    for region in range(regions):
        @pl.when(exists(me + offsets[region]))
        def _():
            ghost_copy(region).wait_send()

        @pl.when(exists(me - offsets[region]))
        def _():
            back_copy(region).wait_send()


def per_device(
    n_curve,
    n_seg,
    solution,
    viscosity,
    slot_index,
    slot_weight,
    mirror_rows,
    ghost_live,
    cell_count,
    viscous_block,
    pressure_block,
):
    owned, width = solution.shape
    elems, slots = slot_index.shape
    regions, ghost_rows = mirror_rows.shape[1:]
    pad_rows = -(-ghost_rows // LANES) * LANES
    columns = owned + regions * ghost_rows
    bf16 = jnp.bfloat16
    i32 = jnp.int32
    f32 = jnp.float32
    return pl.pallas_call(
        functools.partial(operator_kernel, n_curve, n_seg),
        out_shape=jax.ShapeDtypeStruct((owned, width), jnp.float32),
        in_specs=[pl.BlockSpec(memory_space=pltpu.SMEM)]
        + [pl.BlockSpec(memory_space=pltpu.HBM)] * 8,
        out_specs=pl.BlockSpec(memory_space=pltpu.VMEM),
        scratch_shapes=[
            pltpu.VMEM((owned, width), bf16),
            pltpu.VMEM((1, elems), f32),
            pltpu.VMEM((slots, elems), i32),
            pltpu.VMEM((slots, elems), i32),
            pltpu.VMEM((regions, ghost_rows), i32),
            pltpu.VMEM((1, regions), i32),
            pltpu.VMEM((width, width), bf16),
            pltpu.VMEM((width, width), bf16),
            pltpu.VMEM((elems // LANES, columns, LANES), bf16),
            pltpu.VMEM((owned, regions * pad_rows), bf16),
            pltpu.VMEM((width, columns), bf16),
            pltpu.VMEM((width, elems), f32),
            pltpu.VMEM((width, elems), bf16),
            pltpu.VMEM((regions * pad_rows, width), bf16),
            pltpu.VMEM((regions * ghost_rows, width), bf16),
            pltpu.VMEM((regions * ghost_rows, width), bf16),
            pltpu.VMEM((regions * pad_rows, width), bf16),
            pltpu.SemaphoreType.DMA((8,)),
            pltpu.SemaphoreType.DMA((regions,)),
            pltpu.SemaphoreType.DMA((regions,)),
            pltpu.SemaphoreType.DMA((regions,)),
            pltpu.SemaphoreType.DMA((regions,)),
        ],
        compiler_params=pltpu.CompilerParams(
            collective_id=0, has_side_effects=True, vmem_limit_bytes=48 * 1024 * 1024
        ),
    )(
        cell_count,
        *(
            pltpu.with_memory_space_constraint(operand, pltpu.HBM)
            for operand in (
                solution,
                viscosity.reshape(1, elems),
                slot_index.T,
                slot_weight.T,
                mirror_rows.reshape(regions, ghost_rows),
                ghost_live,
                viscous_block,
                pressure_block,
            )
        )
    )


def solution(mesh):
    return jax.shard_map(
        functools.partial(per_device, mesh.shape["curve"], mesh.shape["seg"]),
        mesh=mesh,
        in_specs=(
            P(("curve", "seg"), None),
            P(("curve", "seg")),
            P(("curve", "seg"), None),
            P(("curve", "seg"), None),
            P(("curve", "seg"), None, None),
            P(("curve", "seg"), None),
            P(("curve", "seg")),
            P(),
            P(),
        ),
        out_specs=P(("curve", "seg"), None),
        check_vma=False,
    )
```

```python
import functools

import jax
import jax.numpy as jnp
from jax import lax
from jax.experimental import pallas as pl
from jax.experimental.pallas import tpu as pltpu
from jax.sharding import PartitionSpec as P

LANES = 128
MESH = pl.DeviceIdType.MESH


def shift_list(region_count):
    return [(region // 2 + 1) * (1 if region % 2 == 0 else -1) for region in range(region_count)]


def contract(lhs, rhs, lhs_dim, rhs_dim):
    return lax.dot_general(
        lhs, rhs, (((lhs_dim,), (rhs_dim,)), ((), ())), preferred_element_type=jnp.float32
    )


def operator_kernel(
    n_curve,
    n_seg,
    count_ref,
    solution_hbm,
    visc_hbm,
    index_hbm,
    weight_hbm,
    mirror_hbm,
    live_hbm,
    viscous_hbm,
    pressure_hbm,
    out_ref,
    solution_ref,
    visc_ref,
    index_ref,
    weight_ref,
    mirror_ref,
    live_ref,
    viscous_ref,
    pressure_ref,
    table,
    mirror_table,
    dofs_t,
    gathered,
    element_out,
    outgoing,
    ghosts,
    back_out,
    back_in,
    load_sem,
    send_sem,
    recv_sem,
    back_send_sem,
    back_recv_sem,
):
    owned, width = solution_ref.shape
    regions, ghost_rows = mirror_ref.shape
    slots, elems = index_ref.shape
    groups, columns, lanes_of = table.shape
    pad_rows = mirror_table.shape[1] // regions
    devices = n_curve * n_seg
    offsets = shift_list(regions)
    order = [k for k in range(regions) if offsets[k] > 0]
    half = len(order)
    order = order + [k for k in range(regions) if offsets[k] < 0]
    place_of = {region: pos for pos, region in enumerate(order)}
    split = half * ghost_rows
    me = lax.axis_index("curve") * n_seg + lax.axis_index("seg")

    def place(device):
        return (device // n_seg, lax.rem(device, n_seg))

    def exists(device):
        return jnp.logical_and(device >= 0, device < devices)

    barrier = pltpu.get_barrier_semaphore()
    for offset in offsets:
        @pl.when(exists(me + offset))
        def _():
            pl.semaphore_signal(barrier, inc=1, device_id=place(me + offset), device_id_type=MESH)

    pairs = [
        (mirror_hbm, mirror_ref),
        (live_hbm, live_ref),
        (solution_hbm, solution_ref),
        (index_hbm, index_ref),
        (weight_hbm, weight_ref),
        (visc_hbm, visc_ref),
        (viscous_hbm, viscous_ref),
        (pressure_hbm, pressure_ref),
    ]
    loads = [
        pltpu.make_async_copy(source, target, load_sem.at[pos])
        for pos, (source, target) in enumerate(pairs)
    ]
    for load in loads:
        load.start()

    sub = 16
    row16 = lax.broadcasted_iota(jnp.int32, (sub, lanes_of), 0).astype(jnp.int16)
    one = jnp.ones((sub, lanes_of), jnp.bfloat16)
    zero = jnp.zeros((sub, lanes_of), jnp.bfloat16)

    for load in loads[:3]:
        load.wait()
    for pos, region in enumerate(order):
        for part in range(pad_rows // LANES):
            first = part * LANES
            size = min(LANES, ghost_rows - first)
            entry = lax.broadcasted_iota(jnp.int32, (1, LANES), 1) + first
            picks = mirror_ref[region : region + 1, first : first + size]
            if size < LANES:
                picks = jnp.concatenate([picks, jnp.full((1, LANES - size), -1, jnp.int32)], axis=1)
            limit = jnp.minimum(live_ref[0:1, region : region + 1], ghost_rows)
            picks = jnp.where(entry < limit, picks, -1)
            picks = jnp.broadcast_to(picks, (sub, LANES)).astype(jnp.int16) - row16
            for block in range(owned // sub):
                hit = jnp.where(picks == jnp.int16(block * sub), one, zero)
                start = pos * pad_rows + first
                mirror_table[block * sub : (block + 1) * sub, start : start + LANES] = hit
    dofs_t[:, :owned] = solution_ref[...].astype(jnp.float32).T.astype(jnp.bfloat16)
    listed = contract(dofs_t[:, :owned], mirror_table[...], 1, 0)
    outgoing[...] = listed.T.astype(jnp.bfloat16)

    peers = sum(exists(me + offset).astype(jnp.int32) for offset in offsets)
    pl.semaphore_wait(barrier, peers)

    def ghost_copy(region):
        pos = place_of[region]
        return pltpu.make_async_remote_copy(
            src_ref=outgoing.at[pl.ds(pos * pad_rows, ghost_rows)],
            dst_ref=ghosts.at[pl.ds(pos * ghost_rows, ghost_rows)],
            send_sem=send_sem.at[region],
            recv_sem=recv_sem.at[region],
            device_id=place(me + offsets[region]),
            device_id_type=MESH,
        )

    for region in order:
        @pl.when(exists(me + offsets[region]))
        def _():
            ghost_copy(region).start()

    for pos, region in enumerate(order):
        @pl.when(jnp.logical_not(exists(me - offsets[region])))
        def _():
            ghosts[pos * ghost_rows : (pos + 1) * ghost_rows] = jnp.zeros(
                (ghost_rows, width), jnp.bfloat16
            )

        back_in[pos * pad_rows + ghost_rows : (pos + 1) * pad_rows] = jnp.zeros(
            (pad_rows - ghost_rows, width), jnp.bfloat16
        )

        @pl.when(jnp.logical_not(exists(me + offsets[region])))
        def _():
            back_in[pos * pad_rows : pos * pad_rows + ghost_rows] = jnp.zeros(
                (ghost_rows, width), jnp.bfloat16
            )

    for load in loads[3:5]:
        load.wait()
    per_step = min(4, groups)
    chunk = per_step * lanes_of
    count = count_ref[0]

    def moved(index):
        result = index
        for k in range(regions):
            shift = (place_of[k] - k) * ghost_rows
            if shift:
                low = owned + k * ghost_rows
                inside = jnp.logical_and(index >= low, index < low + ghost_rows)
                result = jnp.where(inside, index + shift, result)
        return result

    def step_lanes(step):
        return pl.ds(step * chunk, chunk) if isinstance(step, int) else pl.ds(
            pl.multiple_of(step * chunk, chunk), chunk
        )

    def rows_of(step, low, high):
        return jnp.concatenate(
            [table[step * per_step + inner, low:high, :] for inner in range(per_step)], axis=1
        )

    def owned_product(step):
        return contract(dofs_t[:, :owned], rows_of(step, 0, owned), 1, 0)

    def build(step):
        for inner in range(per_step):
            group = step * per_step + inner
            start = group * lanes_of
            if not isinstance(step, int):
                start = pl.multiple_of(start, lanes_of)
            lanes = pl.ds(start, lanes_of)
            live = (lax.broadcasted_iota(jnp.int32, (1, lanes_of), 1) + start) < count
            index = [moved(index_ref[slot : slot + 1, lanes]) for slot in range(slots)]
            raw = [
                jnp.where(live, weight_ref[slot : slot + 1, lanes].astype(jnp.float32) * 0.125, 0.0)
                for slot in range(slots)
            ]
            merged = []
            for slot in range(slots):
                value = raw[slot]
                for other in range(slot):
                    value = value + jnp.where(index[other] == index[slot], raw[other], 0.0)
                merged.append(value)
            shape = (sub, lanes_of)
            ids = [jnp.broadcast_to(i, shape).astype(jnp.int16) - row16 for i in index]
            wts = [jnp.broadcast_to(v, shape).astype(jnp.bfloat16) for v in merged]
            for block in range(columns // sub):
                value = zero
                for slot in range(0 if block * sub < owned else 1, slots):
                    value = jnp.where(ids[slot] == jnp.int16(block * sub), wts[slot], value)
                table[group, block * sub : (block + 1) * sub, :] = value

    def build_behind(step, carry):
        product = owned_product(step - 1)
        build(step)
        gathered[:, step_lanes(step - 1)] = product
        return carry

    steps = groups // per_step
    build(0)
    lax.fori_loop(1, steps, build_behind, 0)
    gathered[:, step_lanes(steps - 1)] = owned_product(steps - 1)

    def receive(chosen):
        for region in chosen:
            @pl.when(exists(me - offsets[region]))
            def _():
                ghost_copy(region).wait_recv()

    receive(order[:half])
    middle = owned + split
    dofs_t[:, owned:middle] = ghosts[:split].astype(jnp.float32).T.astype(jnp.bfloat16)

    for step in range(steps):
        gathered[:, step_lanes(step)] += contract(
            dofs_t[:, owned:middle], rows_of(step, owned, middle), 1, 0
        )
    for load in loads[5:]:
        load.wait()
    viscous = viscous_ref[...].astype(jnp.float32).T.astype(jnp.bfloat16)
    pressure = pressure_ref[...].astype(jnp.float32).T.astype(jnp.bfloat16)

    receive(order[half:])
    dofs_t[:, middle:] = ghosts[split:].astype(jnp.float32).T.astype(jnp.bfloat16)

    for step in range(steps):
        lanes = step_lanes(step)
        total = gathered[:, lanes] + contract(
            dofs_t[:, middle:], rows_of(step, middle, columns), 1, 0
        )
        element_in = total.astype(jnp.bfloat16)
        result = contract(viscous, element_in, 1, 0) * visc_ref[:, lanes]
        result = result + contract(pressure, element_in, 1, 0)
        element_out[:, lanes] = result.astype(jnp.bfloat16)

    def back_copy(region):
        pos = place_of[region]
        return pltpu.make_async_remote_copy(
            src_ref=back_out.at[pl.ds(pos * ghost_rows, ghost_rows)],
            dst_ref=back_in.at[pl.ds(pos * pad_rows, ghost_rows)],
            send_sem=back_send_sem.at[region],
            recv_sem=back_recv_sem.at[region],
            device_id=place(me - offsets[region]),
            device_id_type=MESH,
        )

    def scatter(low, high):
        rows = jnp.concatenate([table[group, low:high, :] for group in range(groups)], axis=1)
        return contract(element_out[...], rows, 1, 1).T

    back_out[split:] = scatter(middle, columns).astype(jnp.bfloat16)
    for region in order[half:]:
        @pl.when(exists(me - offsets[region]))
        def _():
            back_copy(region).start()

    back_out[:split] = scatter(owned, middle).astype(jnp.bfloat16)
    for region in order[:half]:
        @pl.when(exists(me - offsets[region]))
        def _():
            back_copy(region).start()

    out_ref[...] = scatter(0, owned)

    for chosen, low in ((order[:half], 0), (order[half:], half * pad_rows)):
        for region in chosen:
            @pl.when(exists(me + offsets[region]))
            def _():
                back_copy(region).wait_recv()

        high = low + half * pad_rows
        out_ref[...] += contract(mirror_table[:, low:high], back_in[low:high], 1, 0)

    for region in range(regions):
        @pl.when(exists(me + offsets[region]))
        def _():
            ghost_copy(region).wait_send()

        @pl.when(exists(me - offsets[region]))
        def _():
            back_copy(region).wait_send()


def per_device(
    n_curve,
    n_seg,
    solution,
    viscosity,
    slot_index,
    slot_weight,
    mirror_rows,
    ghost_live,
    cell_count,
    viscous_block,
    pressure_block,
):
    owned, width = solution.shape
    elems, slots = slot_index.shape
    regions, ghost_rows = mirror_rows.shape[1:]
    pad_rows = -(-ghost_rows // LANES) * LANES
    columns = owned + regions * ghost_rows
    bf16 = jnp.bfloat16
    i32 = jnp.int32
    f32 = jnp.float32
    return pl.pallas_call(
        functools.partial(operator_kernel, n_curve, n_seg),
        out_shape=jax.ShapeDtypeStruct((owned, width), jnp.float32),
        in_specs=[pl.BlockSpec(memory_space=pltpu.SMEM)]
        + [pl.BlockSpec(memory_space=pltpu.HBM)] * 8,
        out_specs=pl.BlockSpec(memory_space=pltpu.VMEM),
        scratch_shapes=[
            pltpu.VMEM((owned, width), bf16),
            pltpu.VMEM((1, elems), f32),
            pltpu.VMEM((slots, elems), i32),
            pltpu.VMEM((slots, elems), i32),
            pltpu.VMEM((regions, ghost_rows), i32),
            pltpu.VMEM((1, regions), i32),
            pltpu.VMEM((width, width), bf16),
            pltpu.VMEM((width, width), bf16),
            pltpu.VMEM((elems // LANES, columns, LANES), bf16),
            pltpu.VMEM((owned, regions * pad_rows), bf16),
            pltpu.VMEM((width, columns), bf16),
            pltpu.VMEM((width, elems), f32),
            pltpu.VMEM((width, elems), bf16),
            pltpu.VMEM((regions * pad_rows, width), bf16),
            pltpu.VMEM((regions * ghost_rows, width), bf16),
            pltpu.VMEM((regions * ghost_rows, width), bf16),
            pltpu.VMEM((regions * pad_rows, width), bf16),
            pltpu.SemaphoreType.DMA((8,)),
            pltpu.SemaphoreType.DMA((regions,)),
            pltpu.SemaphoreType.DMA((regions,)),
            pltpu.SemaphoreType.DMA((regions,)),
            pltpu.SemaphoreType.DMA((regions,)),
        ],
        compiler_params=pltpu.CompilerParams(
            collective_id=0, has_side_effects=True, vmem_limit_bytes=48 * 1024 * 1024
        ),
    )(
        cell_count,
        *(
            pltpu.with_memory_space_constraint(operand, pltpu.HBM)
            for operand in (
                solution,
                viscosity.reshape(1, elems),
                slot_index.T,
                slot_weight.T,
                mirror_rows.reshape(regions, ghost_rows),
                ghost_live,
                viscous_block,
                pressure_block,
            )
        )
    )


def solution(mesh):
    return jax.shard_map(
        functools.partial(per_device, mesh.shape["curve"], mesh.shape["seg"]),
        mesh=mesh,
        in_specs=(
            P(("curve", "seg"), None),
            P(("curve", "seg")),
            P(("curve", "seg"), None),
            P(("curve", "seg"), None),
            P(("curve", "seg"), None, None),
            P(("curve", "seg"), None),
            P(("curve", "seg")),
            P(),
            P(),
        ),
        out_specs=P(("curve", "seg"), None),
        check_vma=False,
    )
```

```python
import functools

import jax
import jax.numpy as jnp
from jax import lax
from jax.experimental import pallas as pl
from jax.experimental.pallas import tpu as pltpu
from jax.sharding import PartitionSpec as P

LANES = 128
ROW = 12
MESH = pl.DeviceIdType.MESH


def shift_list(region_count):
    return [(region // 2 + 1) * (1 if region % 2 == 0 else -1) for region in range(region_count)]


def contract(lhs, rhs, lhs_dim, rhs_dim):
    return lax.dot_general(
        lhs, rhs, (((lhs_dim,), (rhs_dim,)), ((), ())), preferred_element_type=jnp.float32
    )


def operator_kernel(
    n_curve,
    n_seg,
    count_ref,
    solution_hbm,
    visc_hbm,
    index_hbm,
    weight_hbm,
    mirror_hbm,
    live_hbm,
    viscous_hbm,
    pressure_hbm,
    out_ref,
    solution_ref,
    visc_ref,
    index_ref,
    weight_ref,
    mirror_ref,
    live_ref,
    viscous_ref,
    pressure_ref,
    table,
    mirror_table,
    dofs_t,
    gathered,
    element_out,
    outgoing,
    ghosts,
    relay,
    back_out,
    back_in,
    ready_sem,
    late_sem,
    relay_send_sem,
    relay_recv_sem,
    forward_sem,
    load_sem,
    send_sem,
    recv_sem,
    back_send_sem,
    back_recv_sem,
):
    owned, width = solution_ref.shape
    regions, ghost_rows = mirror_ref.shape
    slots, elems = index_ref.shape
    groups, columns, lanes_of = table.shape
    pad_rows = mirror_table.shape[1] // regions
    devices = n_curve * n_seg
    offsets = shift_list(regions)
    order = [k for k in range(regions) if offsets[k] > 0]
    half = len(order)
    order = order + [k for k in range(regions) if offsets[k] < 0]
    place_of = {region: pos for pos, region in enumerate(order)}
    split = half * ghost_rows
    me = lax.axis_index("curve") * n_seg + lax.axis_index("seg")

    def place(device):
        return (device // n_seg, lax.rem(device, n_seg))

    def exists(device):
        return jnp.logical_and(device >= 0, device < devices)

    upper = order[half:]
    reach = max(offsets)
    hop = (ROW - 1) * n_seg

    def last_in_row(device):
        return jnp.logical_and(
            lax.rem(device // n_seg, ROW) == ROW - 1, exists(device)
        )

    def crosses(device, offset):
        inside = jnp.logical_and(last_in_row(device), exists(device + offset))
        return jnp.logical_and(inside, (device + offset) // n_seg != device // n_seg)

    def any_cross(device):
        return crosses(device, reach)

    barrier = pltpu.get_barrier_semaphore()

    def greet(device):
        pl.semaphore_signal(barrier, inc=1, device_id=place(device), device_id_type=MESH)

    for offset in offsets:
        wanted = exists(me + offset)
        if offset > 0:
            wanted = jnp.logical_and(wanted, jnp.logical_not(crosses(me, offset)))

        @pl.when(wanted)
        def _():
            greet(me + offset)

    @pl.when(any_cross(me + hop))
    def _():
        greet(me + hop)

    for region in upper:
        @pl.when(crosses(me + hop, -offsets[region]))
        def _():
            greet(me + hop - offsets[region])

    pairs = [
        (mirror_hbm, mirror_ref),
        (live_hbm, live_ref),
        (solution_hbm, solution_ref),
        (index_hbm, index_ref),
        (weight_hbm, weight_ref),
        (visc_hbm, visc_ref),
        (viscous_hbm, viscous_ref),
        (pressure_hbm, pressure_ref),
    ]
    loads = [
        pltpu.make_async_copy(source, target, load_sem.at[pos])
        for pos, (source, target) in enumerate(pairs)
    ]
    for load in loads:
        load.start()

    sub = 16
    row16 = lax.broadcasted_iota(jnp.int32, (sub, lanes_of), 0).astype(jnp.int16)
    one = jnp.ones((sub, lanes_of), jnp.bfloat16)
    zero = jnp.zeros((sub, lanes_of), jnp.bfloat16)

    for load in loads[:3]:
        load.wait()
    for pos, region in enumerate(order):
        for part in range(pad_rows // LANES):
            first = part * LANES
            size = min(LANES, ghost_rows - first)
            entry = lax.broadcasted_iota(jnp.int32, (1, LANES), 1) + first
            picks = mirror_ref[region : region + 1, first : first + size]
            if size < LANES:
                picks = jnp.concatenate([picks, jnp.full((1, LANES - size), -1, jnp.int32)], axis=1)
            limit = jnp.minimum(live_ref[0:1, region : region + 1], ghost_rows)
            picks = jnp.where(entry < limit, picks, -1)
            picks = jnp.broadcast_to(picks, (sub, LANES)).astype(jnp.int16) - row16
            for block in range(owned // sub):
                hit = jnp.where(picks == jnp.int16(block * sub), one, zero)
                start = pos * pad_rows + first
                mirror_table[block * sub : (block + 1) * sub, start : start + LANES] = hit
    dofs_t[:, :owned] = solution_ref[...].astype(jnp.float32).T.astype(jnp.bfloat16)
    listed = contract(dofs_t[:, :owned], mirror_table[...], 1, 0)
    outgoing[...] = listed.T.astype(jnp.bfloat16)

    peers = any_cross(me).astype(jnp.int32)
    for offset in offsets:
        peers = peers + exists(me + offset).astype(jnp.int32)
    pl.semaphore_wait(barrier, peers)

    @pl.when(any_cross(me))
    def _():
        pl.semaphore_signal(ready_sem, inc=1, device_id=place(me - hop), device_id_type=MESH)

    for region in upper:
        @pl.when(crosses(me, -offsets[region]))
        def _():
            target = place(me - offsets[region])
            pl.semaphore_signal(late_sem, inc=1, device_id=target, device_id_type=MESH)

    def ghost_copy(region):
        pos = place_of[region]
        return pltpu.make_async_remote_copy(
            src_ref=outgoing.at[pl.ds(pos * pad_rows, ghost_rows)],
            dst_ref=ghosts.at[pl.ds(pos * ghost_rows, ghost_rows)],
            send_sem=send_sem.at[region],
            recv_sem=recv_sem.at[region],
            device_id=place(me + offsets[region]),
            device_id_type=MESH,
        )

    def relay_copy(region):
        pos = place_of[region]
        return pltpu.make_async_remote_copy(
            src_ref=outgoing.at[pl.ds(pos * pad_rows, ghost_rows)],
            dst_ref=relay.at[pl.ds((pos - half) * ghost_rows, ghost_rows)],
            send_sem=relay_send_sem.at[region],
            recv_sem=relay_recv_sem.at[region],
            device_id=place(me + offsets[region] - hop),
            device_id_type=MESH,
        )

    def forward_copy(region):
        pos = place_of[region]
        return pltpu.make_async_remote_copy(
            src_ref=relay.at[pl.ds((pos - half) * ghost_rows, ghost_rows)],
            dst_ref=ghosts.at[pl.ds(pos * ghost_rows, ghost_rows)],
            send_sem=forward_sem.at[region],
            recv_sem=recv_sem.at[region],
            device_id=place(me + hop),
            device_id_type=MESH,
        )

    def relayed(region):
        if region not in upper:
            return jnp.bool_(False)
        return crosses(me + offsets[region], -offsets[region])

    def direct(region):
        return jnp.logical_and(exists(me + offsets[region]), jnp.logical_not(relayed(region)))

    for region in order:
        @pl.when(direct(region))
        def _():
            ghost_copy(region).start()

        if region in upper:
            @pl.when(relayed(region))
            def _():
                relay_copy(region).start()

    for pos, region in enumerate(order):
        @pl.when(jnp.logical_not(exists(me - offsets[region])))
        def _():
            ghosts[pos * ghost_rows : (pos + 1) * ghost_rows] = jnp.zeros(
                (ghost_rows, width), jnp.bfloat16
            )

        back_in[pos * pad_rows + ghost_rows : (pos + 1) * pad_rows] = jnp.zeros(
            (pad_rows - ghost_rows, width), jnp.bfloat16
        )

        @pl.when(jnp.logical_not(exists(me + offsets[region])))
        def _():
            back_in[pos * pad_rows : pos * pad_rows + ghost_rows] = jnp.zeros(
                (ghost_rows, width), jnp.bfloat16
            )

    for load in loads[3:5]:
        load.wait()
    per_step = min(4, groups)
    chunk = per_step * lanes_of
    count = count_ref[0]

    def moved(index):
        result = index
        for k in range(regions):
            shift = (place_of[k] - k) * ghost_rows
            if shift:
                low = owned + k * ghost_rows
                inside = jnp.logical_and(index >= low, index < low + ghost_rows)
                result = jnp.where(inside, index + shift, result)
        return result

    def step_lanes(step):
        return pl.ds(step * chunk, chunk) if isinstance(step, int) else pl.ds(
            pl.multiple_of(step * chunk, chunk), chunk
        )

    def rows_of(step, low, high):
        return jnp.concatenate(
            [table[step * per_step + inner, low:high, :] for inner in range(per_step)], axis=1
        )

    def owned_product(step):
        return contract(dofs_t[:, :owned], rows_of(step, 0, owned), 1, 0)

    def build(step):
        for inner in range(per_step):
            group = step * per_step + inner
            start = group * lanes_of
            if not isinstance(step, int):
                start = pl.multiple_of(start, lanes_of)
            lanes = pl.ds(start, lanes_of)
            live = (lax.broadcasted_iota(jnp.int32, (1, lanes_of), 1) + start) < count
            index = [moved(index_ref[slot : slot + 1, lanes]) for slot in range(slots)]
            raw = [
                jnp.where(live, weight_ref[slot : slot + 1, lanes].astype(jnp.float32) * 0.125, 0.0)
                for slot in range(slots)
            ]
            merged = []
            for slot in range(slots):
                value = raw[slot]
                for other in range(slot):
                    value = value + jnp.where(index[other] == index[slot], raw[other], 0.0)
                merged.append(value)
            shape = (sub, lanes_of)
            ids = [jnp.broadcast_to(i, shape).astype(jnp.int16) - row16 for i in index]
            wts = [jnp.broadcast_to(v, shape).astype(jnp.bfloat16) for v in merged]
            for block in range(columns // sub):
                value = zero
                for slot in range(0 if block * sub < owned else 1, slots):
                    value = jnp.where(ids[slot] == jnp.int16(block * sub), wts[slot], value)
                table[group, block * sub : (block + 1) * sub, :] = value

    def build_behind(step, carry):
        product = owned_product(step - 1)
        build(step)
        gathered[:, step_lanes(step - 1)] = product
        return carry

    steps = groups // per_step
    build(0)
    lax.fori_loop(1, steps, build_behind, 0)
    gathered[:, step_lanes(steps - 1)] = owned_product(steps - 1)

    def receive(chosen):
        for region in chosen:
            @pl.when(exists(me - offsets[region]))
            def _():
                ghost_copy(region).wait_recv()

    receive(order[:half])
    middle = owned + split
    dofs_t[:, owned:middle] = ghosts[:split].astype(jnp.float32).T.astype(jnp.bfloat16)

    for step in range(steps):
        gathered[:, step_lanes(step)] += contract(
            dofs_t[:, owned:middle], rows_of(step, owned, middle), 1, 0
        )
    for load in loads[5:]:
        load.wait()
    both = jnp.concatenate(
        [
            viscous_ref[...].astype(jnp.float32).T.astype(jnp.bfloat16),
            pressure_ref[...].astype(jnp.float32).T.astype(jnp.bfloat16),
        ],
        axis=0,
    )

    receive(order[half:])
    dofs_t[:, middle:] = ghosts[split:].astype(jnp.float32).T.astype(jnp.bfloat16)

    for step in range(steps):
        lanes = step_lanes(step)
        total = gathered[:, lanes] + contract(
            dofs_t[:, middle:], rows_of(step, middle, columns), 1, 0
        )
        element_in = total.astype(jnp.bfloat16)
        applied = contract(both, element_in, 1, 0)
        result = applied[:width] * visc_ref[:, lanes] + applied[width:]
        element_out[:, lanes] = result.astype(jnp.bfloat16)

    def back_copy(region):
        pos = place_of[region]
        return pltpu.make_async_remote_copy(
            src_ref=back_out.at[pl.ds(pos * ghost_rows, ghost_rows)],
            dst_ref=back_in.at[pl.ds(pos * pad_rows, ghost_rows)],
            send_sem=back_send_sem.at[region],
            recv_sem=back_recv_sem.at[region],
            device_id=place(me - offsets[region]),
            device_id_type=MESH,
        )

    def scatter(low, high):
        rows = jnp.concatenate([table[group, low:high, :] for group in range(groups)], axis=1)
        return contract(element_out[...], rows, 1, 1).T

    back_out[split:] = scatter(middle, columns).astype(jnp.bfloat16)
    for region in order[half:]:
        @pl.when(exists(me - offsets[region]))
        def _():
            back_copy(region).start()

    back_out[:split] = scatter(owned, middle).astype(jnp.bfloat16)
    late = jnp.int32(0)
    for region in upper:
        late = late + relayed(region).astype(jnp.int32)

    @pl.when(late > 0)
    def _():
        pl.semaphore_wait(late_sem, late)
    for region in order[:half]:
        @pl.when(exists(me - offsets[region]))
        def _():
            back_copy(region).start()

    @pl.when(any_cross(me + hop))
    def _():
        pl.semaphore_wait(ready_sem, 1)

    for region in upper:
        @pl.when(crosses(me + hop, -offsets[region]))
        def _():
            relay_copy(region).wait_recv()
            forward_copy(region).start()

    out_ref[...] = scatter(0, owned)

    for chosen, low in ((order[:half], 0), (order[half:], half * pad_rows)):
        for region in chosen:
            @pl.when(exists(me + offsets[region]))
            def _():
                back_copy(region).wait_recv()

        high = low + half * pad_rows
        out_ref[...] += contract(mirror_table[:, low:high], back_in[low:high], 1, 0)

    for region in range(regions):
        @pl.when(direct(region))
        def _():
            ghost_copy(region).wait_send()

        if region in upper:
            @pl.when(relayed(region))
            def _():
                relay_copy(region).wait_send()

            @pl.when(crosses(me + hop, -offsets[region]))
            def _():
                forward_copy(region).wait_send()

        @pl.when(exists(me - offsets[region]))
        def _():
            back_copy(region).wait_send()


def per_device(
    n_curve,
    n_seg,
    solution,
    viscosity,
    slot_index,
    slot_weight,
    mirror_rows,
    ghost_live,
    cell_count,
    viscous_block,
    pressure_block,
):
    owned, width = solution.shape
    elems, slots = slot_index.shape
    regions, ghost_rows = mirror_rows.shape[1:]
    pad_rows = -(-ghost_rows // LANES) * LANES
    columns = owned + regions * ghost_rows
    bf16 = jnp.bfloat16
    i32 = jnp.int32
    f32 = jnp.float32
    return pl.pallas_call(
        functools.partial(operator_kernel, n_curve, n_seg),
        out_shape=jax.ShapeDtypeStruct((owned, width), jnp.float32),
        in_specs=[pl.BlockSpec(memory_space=pltpu.SMEM)]
        + [pl.BlockSpec(memory_space=pltpu.HBM)] * 8,
        out_specs=pl.BlockSpec(memory_space=pltpu.VMEM),
        scratch_shapes=[
            pltpu.VMEM((owned, width), bf16),
            pltpu.VMEM((1, elems), f32),
            pltpu.VMEM((slots, elems), i32),
            pltpu.VMEM((slots, elems), i32),
            pltpu.VMEM((regions, ghost_rows), i32),
            pltpu.VMEM((1, regions), i32),
            pltpu.VMEM((width, width), bf16),
            pltpu.VMEM((width, width), bf16),
            pltpu.VMEM((elems // LANES, columns, LANES), bf16),
            pltpu.VMEM((owned, regions * pad_rows), bf16),
            pltpu.VMEM((width, columns), bf16),
            pltpu.VMEM((width, elems), f32),
            pltpu.VMEM((width, elems), bf16),
            pltpu.VMEM((regions * pad_rows, width), bf16),
            pltpu.VMEM((regions * ghost_rows, width), bf16),
            pltpu.VMEM((regions // 2 * ghost_rows, width), bf16),
            pltpu.VMEM((regions * ghost_rows, width), bf16),
            pltpu.VMEM((regions * pad_rows, width), bf16),
            pltpu.SemaphoreType.REGULAR,
            pltpu.SemaphoreType.REGULAR,
            pltpu.SemaphoreType.DMA((regions,)),
            pltpu.SemaphoreType.DMA((regions,)),
            pltpu.SemaphoreType.DMA((regions,)),
            pltpu.SemaphoreType.DMA((8,)),
            pltpu.SemaphoreType.DMA((regions,)),
            pltpu.SemaphoreType.DMA((regions,)),
            pltpu.SemaphoreType.DMA((regions,)),
            pltpu.SemaphoreType.DMA((regions,)),
        ],
        compiler_params=pltpu.CompilerParams(
            collective_id=0, has_side_effects=True, vmem_limit_bytes=48 * 1024 * 1024
        ),
    )(
        cell_count,
        *(
            pltpu.with_memory_space_constraint(operand, pltpu.HBM)
            for operand in (
                solution,
                viscosity.reshape(1, elems),
                slot_index.T,
                slot_weight.T,
                mirror_rows.reshape(regions, ghost_rows),
                ghost_live,
                viscous_block,
                pressure_block,
            )
        )
    )


def solution(mesh):
    return jax.shard_map(
        functools.partial(per_device, mesh.shape["curve"], mesh.shape["seg"]),
        mesh=mesh,
        in_specs=(
            P(("curve", "seg"), None),
            P(("curve", "seg")),
            P(("curve", "seg"), None),
            P(("curve", "seg"), None),
            P(("curve", "seg"), None, None),
            P(("curve", "seg"), None),
            P(("curve", "seg")),
            P(),
            P(),
        ),
        out_specs=P(("curve", "seg"), None),
        check_vma=False,
    )
```

```python
import functools

import jax
import jax.numpy as jnp
from jax import lax
from jax.experimental import pallas as pl
from jax.experimental.pallas import tpu as pltpu
from jax.sharding import PartitionSpec as P

LANES = 128
ROW = 12
MESH = pl.DeviceIdType.MESH


def shift_list(region_count):
    return [(region // 2 + 1) * (1 if region % 2 == 0 else -1) for region in range(region_count)]


def contract(lhs, rhs, lhs_dim, rhs_dim):
    return lax.dot_general(
        lhs, rhs, (((lhs_dim,), (rhs_dim,)), ((), ())), preferred_element_type=jnp.float32
    )


def operator_kernel(
    n_curve,
    n_seg,
    count_ref,
    solution_hbm,
    visc_hbm,
    index_hbm,
    weight_hbm,
    mirror_hbm,
    live_hbm,
    viscous_hbm,
    pressure_hbm,
    out_ref,
    solution_ref,
    visc_ref,
    index_ref,
    weight_ref,
    mirror_ref,
    live_ref,
    viscous_ref,
    pressure_ref,
    table,
    mirror_table,
    dofs_t,
    gathered,
    element_out,
    outgoing,
    ghosts,
    relay,
    back_out,
    back_in,
    ready_sem,
    late_sem,
    relay_send_sem,
    relay_recv_sem,
    forward_sem,
    load_sem,
    send_sem,
    recv_sem,
    back_send_sem,
    back_recv_sem,
):
    owned, width = solution_ref.shape
    regions, ghost_rows = mirror_ref.shape
    slots, elems = index_ref.shape
    groups, columns, lanes_of = table.shape
    pad_rows = mirror_table.shape[1] // regions
    devices = n_curve * n_seg
    offsets = shift_list(regions)
    order = [k for k in range(regions) if offsets[k] > 0]
    half = len(order)
    order = order + [k for k in range(regions) if offsets[k] < 0]
    place_of = {region: pos for pos, region in enumerate(order)}
    split = half * ghost_rows
    me = lax.axis_index("curve") * n_seg + lax.axis_index("seg")

    def place(device):
        return (device // n_seg, lax.rem(device, n_seg))

    def exists(device):
        return jnp.logical_and(device >= 0, device < devices)

    upper = order[half:]
    reach = max(offsets)
    hop = (ROW - 1) * n_seg

    def last_in_row(device):
        return jnp.logical_and(
            lax.rem(device // n_seg, ROW) == ROW - 1, exists(device)
        )

    def crosses(device, offset):
        inside = jnp.logical_and(last_in_row(device), exists(device + offset))
        return jnp.logical_and(inside, (device + offset) // n_seg != device // n_seg)

    def any_cross(device):
        return crosses(device, reach)

    barrier = pltpu.get_barrier_semaphore()

    def greet(device):
        pl.semaphore_signal(barrier, inc=1, device_id=place(device), device_id_type=MESH)

    for offset in offsets:
        wanted = exists(me + offset)
        if offset > 0:
            wanted = jnp.logical_and(wanted, jnp.logical_not(crosses(me, offset)))

        @pl.when(wanted)
        def _():
            greet(me + offset)

    @pl.when(any_cross(me + hop))
    def _():
        greet(me + hop)

    for region in upper:
        @pl.when(crosses(me + hop, -offsets[region]))
        def _():
            greet(me + hop - offsets[region])

    pairs = [
        (mirror_hbm, mirror_ref),
        (live_hbm, live_ref),
        (solution_hbm, solution_ref),
        (index_hbm, index_ref),
        (weight_hbm, weight_ref),
        (visc_hbm, visc_ref),
        (viscous_hbm, viscous_ref),
        (pressure_hbm, pressure_ref),
    ]
    loads = [
        pltpu.make_async_copy(source, target, load_sem.at[pos])
        for pos, (source, target) in enumerate(pairs)
    ]
    for load in loads:
        load.start()

    sub = 16
    row16 = lax.broadcasted_iota(jnp.int32, (sub, lanes_of), 0).astype(jnp.int16)
    one = jnp.ones((sub, lanes_of), jnp.bfloat16)
    zero = jnp.zeros((sub, lanes_of), jnp.bfloat16)

    for load in loads[:3]:
        load.wait()
    for pos, region in enumerate(order):
        for part in range(pad_rows // LANES):
            first = part * LANES
            size = min(LANES, ghost_rows - first)
            entry = lax.broadcasted_iota(jnp.int32, (1, LANES), 1) + first
            picks = mirror_ref[region : region + 1, first : first + size]
            if size < LANES:
                picks = jnp.concatenate([picks, jnp.full((1, LANES - size), -1, jnp.int32)], axis=1)
            limit = jnp.minimum(live_ref[0:1, region : region + 1], ghost_rows)
            picks = jnp.where(entry < limit, picks, -1)
            picks = jnp.broadcast_to(picks, (sub, LANES)).astype(jnp.int16) - row16
            for block in range(owned // sub):
                hit = jnp.where(picks == jnp.int16(block * sub), one, zero)
                start = pos * pad_rows + first
                mirror_table[block * sub : (block + 1) * sub, start : start + LANES] = hit
    dofs_t[:, :owned] = solution_ref[...].astype(jnp.float32).T.astype(jnp.bfloat16)
    listed = contract(dofs_t[:, :owned], mirror_table[...], 1, 0)
    outgoing[...] = listed.T.astype(jnp.bfloat16)

    peers = any_cross(me).astype(jnp.int32)
    for offset in offsets:
        peers = peers + exists(me + offset).astype(jnp.int32)
    pl.semaphore_wait(barrier, peers)

    @pl.when(any_cross(me))
    def _():
        pl.semaphore_signal(ready_sem, inc=1, device_id=place(me - hop), device_id_type=MESH)

    for region in upper:
        @pl.when(crosses(me, -offsets[region]))
        def _():
            target = place(me - offsets[region])
            pl.semaphore_signal(late_sem, inc=1, device_id=target, device_id_type=MESH)

    def ghost_copy(region):
        pos = place_of[region]
        return pltpu.make_async_remote_copy(
            src_ref=outgoing.at[pl.ds(pos * pad_rows, ghost_rows)],
            dst_ref=ghosts.at[pl.ds(pos * ghost_rows, ghost_rows)],
            send_sem=send_sem.at[region],
            recv_sem=recv_sem.at[region],
            device_id=place(me + offsets[region]),
            device_id_type=MESH,
        )

    def relay_copy(region):
        pos = place_of[region]
        return pltpu.make_async_remote_copy(
            src_ref=outgoing.at[pl.ds(pos * pad_rows, ghost_rows)],
            dst_ref=relay.at[pl.ds((pos - half) * ghost_rows, ghost_rows)],
            send_sem=relay_send_sem.at[region],
            recv_sem=relay_recv_sem.at[region],
            device_id=place(me + offsets[region] - hop),
            device_id_type=MESH,
        )

    def forward_copy(region):
        pos = place_of[region]
        return pltpu.make_async_remote_copy(
            src_ref=relay.at[pl.ds((pos - half) * ghost_rows, ghost_rows)],
            dst_ref=ghosts.at[pl.ds(pos * ghost_rows, ghost_rows)],
            send_sem=forward_sem.at[region],
            recv_sem=recv_sem.at[region],
            device_id=place(me + hop),
            device_id_type=MESH,
        )

    def relayed(region):
        if region not in upper:
            return jnp.bool_(False)
        return crosses(me + offsets[region], -offsets[region])

    def direct(region):
        return jnp.logical_and(exists(me + offsets[region]), jnp.logical_not(relayed(region)))

    for region in order:
        @pl.when(direct(region))
        def _():
            ghost_copy(region).start()

        if region in upper:
            @pl.when(relayed(region))
            def _():
                relay_copy(region).start()

    for pos, region in enumerate(order):
        @pl.when(jnp.logical_not(exists(me - offsets[region])))
        def _():
            ghosts[pos * ghost_rows : (pos + 1) * ghost_rows] = jnp.zeros(
                (ghost_rows, width), jnp.bfloat16
            )

        back_in[pos * pad_rows + ghost_rows : (pos + 1) * pad_rows] = jnp.zeros(
            (pad_rows - ghost_rows, width), jnp.bfloat16
        )

        @pl.when(jnp.logical_not(exists(me + offsets[region])))
        def _():
            back_in[pos * pad_rows : pos * pad_rows + ghost_rows] = jnp.zeros(
                (ghost_rows, width), jnp.bfloat16
            )

    for load in loads[3:5]:
        load.wait()
    per_step = min(4, groups)
    chunk = per_step * lanes_of
    count = count_ref[0]

    def moved(index):
        result = index
        for k in range(regions):
            shift = (place_of[k] - k) * ghost_rows
            if shift:
                low = owned + k * ghost_rows
                inside = jnp.logical_and(index >= low, index < low + ghost_rows)
                result = jnp.where(inside, index + shift, result)
        return result

    def step_lanes(step):
        return pl.ds(step * chunk, chunk) if isinstance(step, int) else pl.ds(
            pl.multiple_of(step * chunk, chunk), chunk
        )

    def rows_of(step, low, high):
        return jnp.concatenate(
            [table[step * per_step + inner, low:high, :] for inner in range(per_step)], axis=1
        )

    def owned_product(step):
        return contract(dofs_t[:, :owned], rows_of(step, 0, owned), 1, 0)

    span = 64

    def build(step):
        for inner in range(per_step):
            group = step * per_step + inner
            start = group * lanes_of
            if not isinstance(step, int):
                start = pl.multiple_of(start, lanes_of)
            lanes = pl.ds(start, lanes_of)
            live = (lax.broadcasted_iota(jnp.int32, (1, lanes_of), 1) + start) < count
            shape = (sub, lanes_of)
            blocks = []
            patterns = []
            for slot in range(slots):
                index = index_ref[slot : slot + 1, lanes]
                if slot:
                    index = moved(index)
                weight = weight_ref[slot : slot + 1, lanes].astype(jnp.float32) * 0.125
                weight = jnp.broadcast_to(jnp.where(live, weight, 0.0), shape).astype(jnp.bfloat16)
                rest = jnp.broadcast_to(jnp.bitwise_and(index, span - 1), shape).astype(jnp.int16) - row16
                blocks.append(jnp.broadcast_to(jnp.right_shift(index, span.bit_length() - 1), shape).astype(jnp.int16))
                patterns.append(
                    [jnp.where(rest == jnp.int16(part * sub), weight, zero) for part in range(span // sub)]
                )
            summed = []
            for slot in range(slots):
                pattern = patterns[slot]
                for other in range(slot):
                    same = blocks[other] == blocks[slot]
                    pattern = [
                        mine + jnp.where(same, theirs, zero)
                        for mine, theirs in zip(pattern, patterns[other])
                    ]
                summed.append(pattern)
            for block in range(columns // span):
                values = [zero] * (span // sub)
                for slot in range(0 if block * span < owned else 1, slots):
                    match = blocks[slot] == jnp.int16(block)
                    values = [
                        jnp.where(match, mine, value)
                        for mine, value in zip(summed[slot], values)
                    ]
                for part in range(span // sub):
                    row = block * span + part * sub
                    table[group, row : row + sub, :] = values[part]

    def build_behind(step, carry):
        product = owned_product(step - 1)
        build(step)
        gathered[:, step_lanes(step - 1)] = product
        return carry

    steps = groups // per_step
    build(0)
    lax.fori_loop(1, steps, build_behind, 0)
    gathered[:, step_lanes(steps - 1)] = owned_product(steps - 1)

    def receive(chosen):
        for region in chosen:
            @pl.when(exists(me - offsets[region]))
            def _():
                ghost_copy(region).wait_recv()

    receive(order[:half])
    middle = owned + split
    dofs_t[:, owned:middle] = ghosts[:split].astype(jnp.float32).T.astype(jnp.bfloat16)

    for step in range(steps):
        gathered[:, step_lanes(step)] += contract(
            dofs_t[:, owned:middle], rows_of(step, owned, middle), 1, 0
        )
    for load in loads[5:]:
        load.wait()
    both = jnp.concatenate(
        [
            viscous_ref[...].astype(jnp.float32).T.astype(jnp.bfloat16),
            pressure_ref[...].astype(jnp.float32).T.astype(jnp.bfloat16),
        ],
        axis=0,
    )

    receive(order[half:])
    dofs_t[:, middle:] = ghosts[split:].astype(jnp.float32).T.astype(jnp.bfloat16)

    width_of = 4
    pieces = groups // width_of

    def piece_lanes(piece):
        return pl.ds(piece * width_of * lanes_of, width_of * lanes_of)

    def upper_product(piece):
        first = piece * width_of
        rows = [table[first + inner, middle:columns, :] for inner in range(width_of)]
        return contract(dofs_t[:, middle:], jnp.concatenate(rows, axis=1), 1, 0)

    pending = [upper_product(piece) for piece in range(min(1, pieces))]
    for piece in range(pieces):
        if piece + 1 < pieces:
            pending.append(upper_product(piece + 1))
        lanes = piece_lanes(piece)
        element_in = (gathered[:, lanes] + pending[piece]).astype(jnp.bfloat16)
        applied = contract(both, element_in, 1, 0)
        result = applied[:width] * visc_ref[:, lanes] + applied[width:]
        element_out[:, lanes] = result.astype(jnp.bfloat16)

    def back_copy(region):
        pos = place_of[region]
        return pltpu.make_async_remote_copy(
            src_ref=back_out.at[pl.ds(pos * ghost_rows, ghost_rows)],
            dst_ref=back_in.at[pl.ds(pos * pad_rows, ghost_rows)],
            send_sem=back_send_sem.at[region],
            recv_sem=back_recv_sem.at[region],
            device_id=place(me - offsets[region]),
            device_id_type=MESH,
        )

    def scatter(low, high):
        rows = jnp.concatenate([table[group, low:high, :] for group in range(groups)], axis=1)
        return contract(element_out[...], rows, 1, 1).T

    for region in upper[::-1]:
        start = place_of[region] * ghost_rows
        stop = start + ghost_rows
        back_out[start:stop] = scatter(owned + start, owned + stop).astype(jnp.bfloat16)

        @pl.when(exists(me - offsets[region]))
        def _():
            back_copy(region).start()

    back_out[:split] = scatter(owned, middle).astype(jnp.bfloat16)
    late = jnp.int32(0)
    for region in upper:
        late = late + relayed(region).astype(jnp.int32)

    @pl.when(late > 0)
    def _():
        pl.semaphore_wait(late_sem, late)
    for region in order[:half]:
        @pl.when(exists(me - offsets[region]))
        def _():
            back_copy(region).start()

    @pl.when(any_cross(me + hop))
    def _():
        pl.semaphore_wait(ready_sem, 1)

    for region in upper:
        @pl.when(crosses(me + hop, -offsets[region]))
        def _():
            relay_copy(region).wait_recv()
            forward_copy(region).start()

    out_ref[...] = scatter(0, owned)

    for chosen, low in ((order[:half], 0), (order[half:], half * pad_rows)):
        for region in chosen:
            @pl.when(exists(me + offsets[region]))
            def _():
                back_copy(region).wait_recv()

        high = low + half * pad_rows
        out_ref[...] += contract(mirror_table[:, low:high], back_in[low:high], 1, 0)

    for region in range(regions):
        @pl.when(direct(region))
        def _():
            ghost_copy(region).wait_send()

        if region in upper:
            @pl.when(relayed(region))
            def _():
                relay_copy(region).wait_send()

            @pl.when(crosses(me + hop, -offsets[region]))
            def _():
                forward_copy(region).wait_send()

        @pl.when(exists(me - offsets[region]))
        def _():
            back_copy(region).wait_send()


def per_device(
    n_curve,
    n_seg,
    solution,
    viscosity,
    slot_index,
    slot_weight,
    mirror_rows,
    ghost_live,
    cell_count,
    viscous_block,
    pressure_block,
):
    owned, width = solution.shape
    elems, slots = slot_index.shape
    regions, ghost_rows = mirror_rows.shape[1:]
    pad_rows = -(-ghost_rows // LANES) * LANES
    columns = owned + regions * ghost_rows
    bf16 = jnp.bfloat16
    i32 = jnp.int32
    f32 = jnp.float32
    return pl.pallas_call(
        functools.partial(operator_kernel, n_curve, n_seg),
        out_shape=jax.ShapeDtypeStruct((owned, width), jnp.float32),
        in_specs=[pl.BlockSpec(memory_space=pltpu.SMEM)]
        + [pl.BlockSpec(memory_space=pltpu.HBM)] * 8,
        out_specs=pl.BlockSpec(memory_space=pltpu.VMEM),
        scratch_shapes=[
            pltpu.VMEM((owned, width), bf16),
            pltpu.VMEM((1, elems), f32),
            pltpu.VMEM((slots, elems), i32),
            pltpu.VMEM((slots, elems), i32),
            pltpu.VMEM((regions, ghost_rows), i32),
            pltpu.VMEM((1, regions), i32),
            pltpu.VMEM((width, width), bf16),
            pltpu.VMEM((width, width), bf16),
            pltpu.VMEM((elems // LANES, columns, LANES), bf16),
            pltpu.VMEM((owned, regions * pad_rows), bf16),
            pltpu.VMEM((width, columns), bf16),
            pltpu.VMEM((width, elems), f32),
            pltpu.VMEM((width, elems), bf16),
            pltpu.VMEM((regions * pad_rows, width), bf16),
            pltpu.VMEM((regions * ghost_rows, width), bf16),
            pltpu.VMEM((regions // 2 * ghost_rows, width), bf16),
            pltpu.VMEM((regions * ghost_rows, width), bf16),
            pltpu.VMEM((regions * pad_rows, width), bf16),
            pltpu.SemaphoreType.REGULAR,
            pltpu.SemaphoreType.REGULAR,
            pltpu.SemaphoreType.DMA((regions,)),
            pltpu.SemaphoreType.DMA((regions,)),
            pltpu.SemaphoreType.DMA((regions,)),
            pltpu.SemaphoreType.DMA((8,)),
            pltpu.SemaphoreType.DMA((regions,)),
            pltpu.SemaphoreType.DMA((regions,)),
            pltpu.SemaphoreType.DMA((regions,)),
            pltpu.SemaphoreType.DMA((regions,)),
        ],
        compiler_params=pltpu.CompilerParams(
            collective_id=0, has_side_effects=True, vmem_limit_bytes=48 * 1024 * 1024
        ),
    )(
        cell_count,
        *(
            pltpu.with_memory_space_constraint(operand, pltpu.HBM)
            for operand in (
                solution,
                viscosity.reshape(1, elems),
                slot_index.T,
                slot_weight.T,
                mirror_rows.reshape(regions, ghost_rows),
                ghost_live,
                viscous_block,
                pressure_block,
            )
        )
    )


def solution(mesh):
    return jax.shard_map(
        functools.partial(per_device, mesh.shape["curve"], mesh.shape["seg"]),
        mesh=mesh,
        in_specs=(
            P(("curve", "seg"), None),
            P(("curve", "seg")),
            P(("curve", "seg"), None),
            P(("curve", "seg"), None),
            P(("curve", "seg"), None, None),
            P(("curve", "seg"), None),
            P(("curve", "seg")),
            P(),
            P(),
        ),
        out_specs=P(("curve", "seg"), None),
        check_vma=False,
    )
```

```python
import functools

import jax
import jax.numpy as jnp
from jax import lax
from jax.experimental import pallas as pl
from jax.experimental.pallas import tpu as pltpu
from jax.sharding import PartitionSpec as P

LANES = 128
PIECE = 192
ROW = 12
MESH = pl.DeviceIdType.MESH


def shift_list(region_count):
    return [(region // 2 + 1) * (1 if region % 2 == 0 else -1) for region in range(region_count)]


def contract(lhs, rhs, lhs_dim, rhs_dim):
    return lax.dot_general(
        lhs, rhs, (((lhs_dim,), (rhs_dim,)), ((), ())), preferred_element_type=jnp.float32
    )


def operator_kernel(
    n_curve,
    n_seg,
    count_ref,
    solution_hbm,
    visc_hbm,
    index_hbm,
    weight_hbm,
    mirror_hbm,
    live_hbm,
    viscous_hbm,
    pressure_hbm,
    out_ref,
    solution_ref,
    visc_ref,
    index_ref,
    weight_ref,
    mirror_ref,
    live_ref,
    viscous_ref,
    pressure_ref,
    table,
    mirror_table,
    dofs_t,
    gathered,
    element_out,
    outgoing,
    ghosts,
    relay,
    back_out,
    back_in,
    ready_sem,
    late_sem,
    relay_send_sem,
    relay_recv_sem,
    forward_sem,
    load_sem,
    send_sem,
    recv_sem,
    back_send_sem,
    back_recv_sem,
):
    owned, width = solution_ref.shape
    regions, ghost_rows = mirror_ref.shape
    slots, elems = index_ref.shape
    groups, columns, lanes_of = table.shape
    pad_rows = mirror_table.shape[1] // regions
    devices = n_curve * n_seg
    offsets = shift_list(regions)
    order = [k for k in range(regions) if offsets[k] > 0]
    half = len(order)
    order = order + [k for k in range(regions) if offsets[k] < 0]
    place_of = {region: pos for pos, region in enumerate(order)}
    split = half * ghost_rows
    me = lax.axis_index("curve") * n_seg + lax.axis_index("seg")

    def place(device):
        return (device // n_seg, lax.rem(device, n_seg))

    def exists(device):
        return jnp.logical_and(device >= 0, device < devices)

    upper = order[half:]
    reach = max(offsets)
    hop = (ROW - 1) * n_seg

    def last_in_row(device):
        return jnp.logical_and(
            lax.rem(device // n_seg, ROW) == ROW - 1, exists(device)
        )

    def crosses(device, offset):
        inside = jnp.logical_and(last_in_row(device), exists(device + offset))
        return jnp.logical_and(inside, (device + offset) // n_seg != device // n_seg)

    def any_cross(device):
        return crosses(device, reach)

    barrier = pltpu.get_barrier_semaphore()

    def greet(device):
        pl.semaphore_signal(barrier, inc=1, device_id=place(device), device_id_type=MESH)

    for offset in offsets:
        wanted = exists(me + offset)
        if offset > 0:
            wanted = jnp.logical_and(wanted, jnp.logical_not(crosses(me, offset)))

        @pl.when(wanted)
        def _():
            greet(me + offset)

    @pl.when(any_cross(me + hop))
    def _():
        greet(me + hop)

    for region in upper:
        @pl.when(crosses(me + hop, -offsets[region]))
        def _():
            greet(me + hop - offsets[region])

    pairs = [
        (mirror_hbm, mirror_ref),
        (live_hbm, live_ref),
        (solution_hbm, solution_ref),
        (index_hbm, index_ref),
        (weight_hbm, weight_ref),
        (visc_hbm, visc_ref),
        (viscous_hbm, viscous_ref),
        (pressure_hbm, pressure_ref),
    ]
    loads = [
        pltpu.make_async_copy(source, target, load_sem.at[pos])
        for pos, (source, target) in enumerate(pairs)
    ]
    for load in loads:
        load.start()

    sub = 16
    row16 = lax.broadcasted_iota(jnp.int32, (sub, lanes_of), 0).astype(jnp.int16)
    one = jnp.ones((sub, lanes_of), jnp.bfloat16)
    zero = jnp.zeros((sub, lanes_of), jnp.bfloat16)

    for load in loads[:3]:
        load.wait()
    for pos, region in enumerate(order):
        for part in range(pad_rows // LANES):
            first = part * LANES
            size = min(LANES, ghost_rows - first)
            entry = lax.broadcasted_iota(jnp.int32, (1, LANES), 1) + first
            picks = mirror_ref[region : region + 1, first : first + size]
            if size < LANES:
                picks = jnp.concatenate([picks, jnp.full((1, LANES - size), -1, jnp.int32)], axis=1)
            limit = jnp.minimum(live_ref[0:1, region : region + 1], ghost_rows)
            picks = jnp.where(entry < limit, picks, -1)
            picks = jnp.broadcast_to(picks, (sub, LANES)).astype(jnp.int16) - row16
            for block in range(owned // sub):
                hit = jnp.where(picks == jnp.int16(block * sub), one, zero)
                start = pos * pad_rows + first
                mirror_table[block * sub : (block + 1) * sub, start : start + LANES] = hit
    dofs_t[:, :owned] = solution_ref[...].astype(jnp.float32).T.astype(jnp.bfloat16)
    listed = contract(dofs_t[:, :owned], mirror_table[...], 1, 0)
    outgoing[...] = listed.T.astype(jnp.bfloat16)

    peers = any_cross(me).astype(jnp.int32)
    for offset in offsets:
        peers = peers + exists(me + offset).astype(jnp.int32)
    pl.semaphore_wait(barrier, peers)

    @pl.when(any_cross(me))
    def _():
        pl.semaphore_signal(ready_sem, inc=1, device_id=place(me - hop), device_id_type=MESH)

    for region in upper:
        @pl.when(crosses(me, -offsets[region]))
        def _():
            target = place(me - offsets[region])
            pl.semaphore_signal(late_sem, inc=1, device_id=target, device_id_type=MESH)

    def ghost_copy(region):
        pos = place_of[region]
        return pltpu.make_async_remote_copy(
            src_ref=outgoing.at[pl.ds(pos * pad_rows, ghost_rows)],
            dst_ref=ghosts.at[pl.ds(pos * ghost_rows, ghost_rows)],
            send_sem=send_sem.at[region],
            recv_sem=recv_sem.at[region],
            device_id=place(me + offsets[region]),
            device_id_type=MESH,
        )

    def relay_copy(region):
        pos = place_of[region]
        return pltpu.make_async_remote_copy(
            src_ref=outgoing.at[pl.ds(pos * pad_rows, ghost_rows)],
            dst_ref=relay.at[pl.ds((pos - half) * ghost_rows, ghost_rows)],
            send_sem=relay_send_sem.at[region],
            recv_sem=relay_recv_sem.at[region],
            device_id=place(me + offsets[region] - hop),
            device_id_type=MESH,
        )

    def forward_copy(region):
        pos = place_of[region]
        return pltpu.make_async_remote_copy(
            src_ref=relay.at[pl.ds((pos - half) * ghost_rows, ghost_rows)],
            dst_ref=ghosts.at[pl.ds(pos * ghost_rows, ghost_rows)],
            send_sem=forward_sem.at[region],
            recv_sem=recv_sem.at[region],
            device_id=place(me + hop),
            device_id_type=MESH,
        )

    def relayed(region):
        if region not in upper:
            return jnp.bool_(False)
        return crosses(me + offsets[region], -offsets[region])

    def direct(region):
        return jnp.logical_and(exists(me + offsets[region]), jnp.logical_not(relayed(region)))

    for region in order:
        @pl.when(direct(region))
        def _():
            ghost_copy(region).start()

        if region in upper:
            @pl.when(relayed(region))
            def _():
                relay_copy(region).start()

    for pos, region in enumerate(order):
        @pl.when(jnp.logical_not(exists(me - offsets[region])))
        def _():
            ghosts[pos * ghost_rows : (pos + 1) * ghost_rows] = jnp.zeros(
                (ghost_rows, width), jnp.bfloat16
            )

        back_in[pos * pad_rows + ghost_rows : (pos + 1) * pad_rows] = jnp.zeros(
            (pad_rows - ghost_rows, width), jnp.bfloat16
        )

        @pl.when(jnp.logical_not(exists(me + offsets[region])))
        def _():
            back_in[pos * pad_rows : pos * pad_rows + ghost_rows] = jnp.zeros(
                (ghost_rows, width), jnp.bfloat16
            )

    for load in loads[3:5]:
        load.wait()
    per_step = min(4, groups)
    chunk = per_step * lanes_of
    count = count_ref[0]

    def moved(index):
        result = index
        for k in range(regions):
            shift = (place_of[k] - k) * ghost_rows
            if shift:
                low = owned + k * ghost_rows
                inside = jnp.logical_and(index >= low, index < low + ghost_rows)
                result = jnp.where(inside, index + shift, result)
        return result

    def step_lanes(step):
        return pl.ds(step * chunk, chunk) if isinstance(step, int) else pl.ds(
            pl.multiple_of(step * chunk, chunk), chunk
        )

    def rows_of(step, low, high):
        return jnp.concatenate(
            [table[step * per_step + inner, low:high, :] for inner in range(per_step)], axis=1
        )

    def owned_product(step):
        return contract(dofs_t[:, :owned], rows_of(step, 0, owned), 1, 0)

    span = 64

    def build(step):
        for inner in range(per_step):
            group = step * per_step + inner
            start = group * lanes_of
            if not isinstance(step, int):
                start = pl.multiple_of(start, lanes_of)
            lanes = pl.ds(start, lanes_of)
            live = (lax.broadcasted_iota(jnp.int32, (1, lanes_of), 1) + start) < count
            shape = (sub, lanes_of)
            blocks = []
            patterns = []
            for slot in range(slots):
                index = index_ref[slot : slot + 1, lanes]
                if slot:
                    index = moved(index)
                weight = weight_ref[slot : slot + 1, lanes].astype(jnp.float32) * 0.125
                weight = jnp.broadcast_to(jnp.where(live, weight, 0.0), shape).astype(jnp.bfloat16)
                rest = jnp.broadcast_to(jnp.bitwise_and(index, span - 1), shape).astype(jnp.int16) - row16
                blocks.append(jnp.broadcast_to(jnp.right_shift(index, span.bit_length() - 1), shape).astype(jnp.int16))
                patterns.append(
                    [jnp.where(rest == jnp.int16(part * sub), weight, zero) for part in range(span // sub)]
                )
            summed = []
            for slot in range(slots):
                pattern = patterns[slot]
                for other in range(slot):
                    same = blocks[other] == blocks[slot]
                    pattern = [
                        mine + jnp.where(same, theirs, zero)
                        for mine, theirs in zip(pattern, patterns[other])
                    ]
                summed.append(pattern)
            for block in range(columns // span):
                values = [zero] * (span // sub)
                for slot in range(0 if block * span < owned else 1, slots):
                    match = blocks[slot] == jnp.int16(block)
                    values = [
                        jnp.where(match, mine, value)
                        for mine, value in zip(summed[slot], values)
                    ]
                for part in range(span // sub):
                    row = block * span + part * sub
                    table[group, row : row + sub, :] = values[part]

    def build_behind(step, carry):
        product = owned_product(step - 1)
        build(step)
        gathered[:, step_lanes(step - 1)] = product
        return carry

    steps = groups // per_step
    build(0)
    lax.fori_loop(1, steps, build_behind, 0)
    gathered[:, step_lanes(steps - 1)] = owned_product(steps - 1)

    def receive(chosen):
        for region in chosen:
            @pl.when(exists(me - offsets[region]))
            def _():
                ghost_copy(region).wait_recv()

    receive(order[:half])
    middle = owned + split
    dofs_t[:, owned:middle] = ghosts[:split].astype(jnp.float32).T.astype(jnp.bfloat16)

    for step in range(steps):
        gathered[:, step_lanes(step)] += contract(
            dofs_t[:, owned:middle], rows_of(step, owned, middle), 1, 0
        )
    for load in loads[5:]:
        load.wait()
    both = jnp.concatenate(
        [
            viscous_ref[...].astype(jnp.float32).T.astype(jnp.bfloat16),
            pressure_ref[...].astype(jnp.float32).T.astype(jnp.bfloat16),
        ],
        axis=0,
    )

    receive(order[half:])
    dofs_t[:, middle:] = ghosts[split:].astype(jnp.float32).T.astype(jnp.bfloat16)

    width_of = per_step
    pieces = groups // width_of

    def piece_lanes(piece):
        return pl.ds(piece * width_of * lanes_of, width_of * lanes_of)

    def upper_product(piece):
        first = piece * width_of
        rows = [table[first + inner, middle:columns, :] for inner in range(width_of)]
        return contract(dofs_t[:, middle:], jnp.concatenate(rows, axis=1), 1, 0)

    pending = [upper_product(piece) for piece in range(min(1, pieces))]
    for piece in range(pieces):
        if piece + 1 < pieces:
            pending.append(upper_product(piece + 1))
        lanes = piece_lanes(piece)
        element_in = (gathered[:, lanes] + pending[piece]).astype(jnp.bfloat16)
        applied = contract(both, element_in, 1, 0)
        result = applied[:width] * visc_ref[:, lanes] + applied[width:]
        element_out[lanes, :] = result.T.astype(jnp.bfloat16)

    def back_copy(region):
        pos = place_of[region]
        return pltpu.make_async_remote_copy(
            src_ref=back_out.at[pl.ds(pos * ghost_rows, ghost_rows)],
            dst_ref=back_in.at[pl.ds(pos * pad_rows, ghost_rows)],
            send_sem=back_send_sem.at[region],
            recv_sem=back_recv_sem.at[region],
            device_id=place(me - offsets[region]),
            device_id_type=MESH,
        )

    def scatter(low, high):
        rows = jnp.concatenate([table[group, low:high, :] for group in range(groups)], axis=1)
        return contract(rows, element_out[...], 1, 0)

    for region in upper[::-1]:
        start = place_of[region] * ghost_rows
        stop = start + ghost_rows
        back_out[start:stop] = scatter(owned + start, owned + stop).astype(jnp.bfloat16)

        @pl.when(exists(me - offsets[region]))
        def _():
            back_copy(region).start()

    late = jnp.int32(0)
    for region in upper:
        late = late + relayed(region).astype(jnp.int32)

    @pl.when(late > 0)
    def _():
        pl.semaphore_wait(late_sem, late)
    for region in order[:half]:
        start = place_of[region] * ghost_rows
        stop = start + ghost_rows
        back_out[start:stop] = scatter(owned + start, owned + stop).astype(jnp.bfloat16)

        @pl.when(exists(me - offsets[region]))
        def _():
            back_copy(region).start()

    @pl.when(any_cross(me + hop))
    def _():
        pl.semaphore_wait(ready_sem, 1)

    for region in upper:
        @pl.when(crosses(me + hop, -offsets[region]))
        def _():
            relay_copy(region).wait_recv()
            forward_copy(region).start()

    for start in range(0, owned, PIECE):
        stop = min(start + PIECE, owned)
        out_ref[start:stop] = scatter(start, stop)

    for chosen, low in ((order[:half], 0), (order[half:], half * pad_rows)):
        for region in chosen:
            @pl.when(exists(me + offsets[region]))
            def _():
                back_copy(region).wait_recv()

        high = low + half * pad_rows
        out_ref[...] += contract(mirror_table[:, low:high], back_in[low:high], 1, 0)

    for region in range(regions):
        @pl.when(direct(region))
        def _():
            ghost_copy(region).wait_send()

        if region in upper:
            @pl.when(relayed(region))
            def _():
                relay_copy(region).wait_send()

            @pl.when(crosses(me + hop, -offsets[region]))
            def _():
                forward_copy(region).wait_send()

        @pl.when(exists(me - offsets[region]))
        def _():
            back_copy(region).wait_send()


def per_device(
    n_curve,
    n_seg,
    solution,
    viscosity,
    slot_index,
    slot_weight,
    mirror_rows,
    ghost_live,
    cell_count,
    viscous_block,
    pressure_block,
):
    owned, width = solution.shape
    elems, slots = slot_index.shape
    regions, ghost_rows = mirror_rows.shape[1:]
    pad_rows = -(-ghost_rows // LANES) * LANES
    columns = owned + regions * ghost_rows
    bf16 = jnp.bfloat16
    i32 = jnp.int32
    f32 = jnp.float32
    return pl.pallas_call(
        functools.partial(operator_kernel, n_curve, n_seg),
        out_shape=jax.ShapeDtypeStruct((owned, width), jnp.float32),
        in_specs=[pl.BlockSpec(memory_space=pltpu.SMEM)]
        + [pl.BlockSpec(memory_space=pltpu.HBM)] * 8,
        out_specs=pl.BlockSpec(memory_space=pltpu.VMEM),
        scratch_shapes=[
            pltpu.VMEM((owned, width), bf16),
            pltpu.VMEM((1, elems), f32),
            pltpu.VMEM((slots, elems), i32),
            pltpu.VMEM((slots, elems), i32),
            pltpu.VMEM((regions, ghost_rows), i32),
            pltpu.VMEM((1, regions), i32),
            pltpu.VMEM((width, width), bf16),
            pltpu.VMEM((width, width), bf16),
            pltpu.VMEM((elems // LANES, columns, LANES), bf16),
            pltpu.VMEM((owned, regions * pad_rows), bf16),
            pltpu.VMEM((width, columns), bf16),
            pltpu.VMEM((width, elems), f32),
            pltpu.VMEM((elems, width), bf16),
            pltpu.VMEM((regions * pad_rows, width), bf16),
            pltpu.VMEM((regions * ghost_rows, width), bf16),
            pltpu.VMEM((regions // 2 * ghost_rows, width), bf16),
            pltpu.VMEM((regions * ghost_rows, width), bf16),
            pltpu.VMEM((regions * pad_rows, width), bf16),
            pltpu.SemaphoreType.REGULAR,
            pltpu.SemaphoreType.REGULAR,
            pltpu.SemaphoreType.DMA((regions,)),
            pltpu.SemaphoreType.DMA((regions,)),
            pltpu.SemaphoreType.DMA((regions,)),
            pltpu.SemaphoreType.DMA((8,)),
            pltpu.SemaphoreType.DMA((regions,)),
            pltpu.SemaphoreType.DMA((regions,)),
            pltpu.SemaphoreType.DMA((regions,)),
            pltpu.SemaphoreType.DMA((regions,)),
        ],
        compiler_params=pltpu.CompilerParams(
            collective_id=0, has_side_effects=True, vmem_limit_bytes=48 * 1024 * 1024
        ),
    )(
        cell_count,
        *(
            pltpu.with_memory_space_constraint(operand, pltpu.HBM)
            for operand in (
                solution,
                viscosity.reshape(1, elems),
                slot_index.T,
                slot_weight.T,
                mirror_rows.reshape(regions, ghost_rows),
                ghost_live,
                viscous_block,
                pressure_block,
            )
        )
    )


def solution(mesh):
    return jax.shard_map(
        functools.partial(per_device, mesh.shape["curve"], mesh.shape["seg"]),
        mesh=mesh,
        in_specs=(
            P(("curve", "seg"), None),
            P(("curve", "seg")),
            P(("curve", "seg"), None),
            P(("curve", "seg"), None),
            P(("curve", "seg"), None, None),
            P(("curve", "seg"), None),
            P(("curve", "seg")),
            P(),
            P(),
        ),
        out_specs=P(("curve", "seg"), None),
        check_vma=False,
    )
```

```python
import functools

import jax
import jax.numpy as jnp
from jax import lax
from jax.experimental import pallas as pl
from jax.experimental.pallas import tpu as pltpu
from jax.sharding import PartitionSpec as P

LANES = 128
PIECE = 192
ROW = 12
MESH = pl.DeviceIdType.MESH


def shift_list(region_count):
    return [(region // 2 + 1) * (1 if region % 2 == 0 else -1) for region in range(region_count)]


def contract(lhs, rhs, lhs_dim, rhs_dim):
    return lax.dot_general(
        lhs, rhs, (((lhs_dim,), (rhs_dim,)), ((), ())), preferred_element_type=jnp.float32
    )


def operator_kernel(
    n_curve,
    n_seg,
    count_ref,
    solution_hbm,
    visc_hbm,
    index_hbm,
    weight_hbm,
    mirror_hbm,
    live_hbm,
    viscous_hbm,
    pressure_hbm,
    out_ref,
    solution_ref,
    visc_ref,
    index_ref,
    weight_ref,
    mirror_ref,
    live_ref,
    viscous_ref,
    pressure_ref,
    table,
    mirror_table,
    dofs_t,
    gathered,
    element_out,
    outgoing,
    ghosts,
    relay,
    back_out,
    back_in,
    ready_sem,
    late_sem,
    relay_send_sem,
    relay_recv_sem,
    forward_sem,
    load_sem,
    send_sem,
    recv_sem,
    back_send_sem,
    back_recv_sem,
):
    owned, width = solution_ref.shape
    regions, ghost_rows = mirror_ref.shape
    slots, elems = index_ref.shape
    groups, columns, lanes_of = table.shape
    pad_rows = mirror_table.shape[1] // regions
    devices = n_curve * n_seg
    offsets = shift_list(regions)
    order = [k for k in range(regions) if offsets[k] > 0]
    half = len(order)
    order = order + [k for k in range(regions) if offsets[k] < 0]
    place_of = {region: pos for pos, region in enumerate(order)}
    split = half * ghost_rows
    me = lax.axis_index("curve") * n_seg + lax.axis_index("seg")

    def place(device):
        return (device // n_seg, lax.rem(device, n_seg))

    def exists(device):
        return jnp.logical_and(device >= 0, device < devices)

    upper = order[half:]
    reach = max(offsets)
    hop = (ROW - 1) * n_seg

    def last_in_row(device):
        return jnp.logical_and(
            lax.rem(device // n_seg, ROW) == ROW - 1, exists(device)
        )

    def crosses(device, offset):
        inside = jnp.logical_and(last_in_row(device), exists(device + offset))
        return jnp.logical_and(inside, (device + offset) // n_seg != device // n_seg)

    def any_cross(device):
        return crosses(device, reach)

    pairs = [
        (mirror_hbm, mirror_ref),
        (live_hbm, live_ref),
        (solution_hbm, solution_ref),
        (index_hbm, index_ref),
        (weight_hbm, weight_ref),
        (visc_hbm, visc_ref),
        (viscous_hbm, viscous_ref),
        (pressure_hbm, pressure_ref),
    ]
    loads = [
        pltpu.make_async_copy(source, target, load_sem.at[pos])
        for pos, (source, target) in enumerate(pairs)
    ]
    for load in loads:
        load.start()

    barrier = pltpu.get_barrier_semaphore()

    def greet(device):
        pl.semaphore_signal(barrier, inc=1, device_id=place(device), device_id_type=MESH)

    for offset in offsets:
        wanted = exists(me + offset)
        if offset > 0:
            wanted = jnp.logical_and(wanted, jnp.logical_not(crosses(me, offset)))

        @pl.when(wanted)
        def _():
            greet(me + offset)

    @pl.when(any_cross(me + hop))
    def _():
        greet(me + hop)

    for region in upper:
        @pl.when(crosses(me + hop, -offsets[region]))
        def _():
            greet(me + hop - offsets[region])

    sub = 16
    row16 = lax.broadcasted_iota(jnp.int32, (sub, lanes_of), 0).astype(jnp.int16)
    one = jnp.ones((sub, lanes_of), jnp.bfloat16)
    zero = jnp.zeros((sub, lanes_of), jnp.bfloat16)

    for load in loads[:3]:
        load.wait()
    for pos, region in enumerate(order):
        for part in range(pad_rows // LANES):
            first = part * LANES
            size = min(LANES, ghost_rows - first)
            entry = lax.broadcasted_iota(jnp.int32, (1, LANES), 1) + first
            picks = mirror_ref[region : region + 1, first : first + size]
            if size < LANES:
                picks = jnp.concatenate([picks, jnp.full((1, LANES - size), -1, jnp.int32)], axis=1)
            limit = jnp.minimum(live_ref[0:1, region : region + 1], ghost_rows)
            picks = jnp.where(entry < limit, picks, -1)
            picks = jnp.broadcast_to(picks, (sub, LANES)).astype(jnp.int16) - row16
            for block in range(owned // sub):
                hit = jnp.where(picks == jnp.int16(block * sub), one, zero)
                start = pos * pad_rows + first
                mirror_table[block * sub : (block + 1) * sub, start : start + LANES] = hit
    peers = any_cross(me).astype(jnp.int32)
    for offset in offsets:
        peers = peers + exists(me + offset).astype(jnp.int32)
    pl.semaphore_wait(barrier, peers)

    @pl.when(any_cross(me))
    def _():
        pl.semaphore_signal(ready_sem, inc=1, device_id=place(me - hop), device_id_type=MESH)

    for region in upper:
        @pl.when(crosses(me, -offsets[region]))
        def _():
            target = place(me - offsets[region])
            pl.semaphore_signal(late_sem, inc=1, device_id=target, device_id_type=MESH)

    dofs_t[:, :owned] = solution_ref[...].astype(jnp.float32).T.astype(jnp.bfloat16)
    listed = contract(dofs_t[:, :owned], mirror_table[...], 1, 0)
    outgoing[...] = listed.T.astype(jnp.bfloat16)

    def ghost_copy(region):
        pos = place_of[region]
        return pltpu.make_async_remote_copy(
            src_ref=outgoing.at[pl.ds(pos * pad_rows, ghost_rows)],
            dst_ref=ghosts.at[pl.ds(pos * ghost_rows, ghost_rows)],
            send_sem=send_sem.at[region],
            recv_sem=recv_sem.at[region],
            device_id=place(me + offsets[region]),
            device_id_type=MESH,
        )

    def relay_copy(region):
        pos = place_of[region]
        return pltpu.make_async_remote_copy(
            src_ref=outgoing.at[pl.ds(pos * pad_rows, ghost_rows)],
            dst_ref=relay.at[pl.ds((pos - half) * ghost_rows, ghost_rows)],
            send_sem=relay_send_sem.at[region],
            recv_sem=relay_recv_sem.at[region],
            device_id=place(me + offsets[region] - hop),
            device_id_type=MESH,
        )

    def forward_copy(region):
        pos = place_of[region]
        return pltpu.make_async_remote_copy(
            src_ref=relay.at[pl.ds((pos - half) * ghost_rows, ghost_rows)],
            dst_ref=ghosts.at[pl.ds(pos * ghost_rows, ghost_rows)],
            send_sem=forward_sem.at[region],
            recv_sem=recv_sem.at[region],
            device_id=place(me + hop),
            device_id_type=MESH,
        )

    def relayed(region):
        if region not in upper:
            return jnp.bool_(False)
        return crosses(me + offsets[region], -offsets[region])

    def direct(region):
        return jnp.logical_and(exists(me + offsets[region]), jnp.logical_not(relayed(region)))

    for region in order:
        @pl.when(direct(region))
        def _():
            ghost_copy(region).start()

        if region in upper:
            @pl.when(relayed(region))
            def _():
                relay_copy(region).start()

    for pos, region in enumerate(order):
        @pl.when(jnp.logical_not(exists(me - offsets[region])))
        def _():
            ghosts[pos * ghost_rows : (pos + 1) * ghost_rows] = jnp.zeros(
                (ghost_rows, width), jnp.bfloat16
            )

        back_in[pos * pad_rows + ghost_rows : (pos + 1) * pad_rows] = jnp.zeros(
            (pad_rows - ghost_rows, width), jnp.bfloat16
        )

        @pl.when(jnp.logical_not(exists(me + offsets[region])))
        def _():
            back_in[pos * pad_rows : pos * pad_rows + ghost_rows] = jnp.zeros(
                (ghost_rows, width), jnp.bfloat16
            )

    for load in loads[3:5]:
        load.wait()
    per_step = min(4, groups)
    chunk = per_step * lanes_of
    count = count_ref[0]

    def moved(index):
        result = index
        for k in range(regions):
            shift = (place_of[k] - k) * ghost_rows
            if shift:
                low = owned + k * ghost_rows
                inside = jnp.logical_and(index >= low, index < low + ghost_rows)
                result = jnp.where(inside, index + shift, result)
        return result

    def step_lanes(step):
        return pl.ds(step * chunk, chunk) if isinstance(step, int) else pl.ds(
            pl.multiple_of(step * chunk, chunk), chunk
        )

    def rows_of(step, low, high):
        return jnp.concatenate(
            [table[step * per_step + inner, low:high, :] for inner in range(per_step)], axis=1
        )

    def owned_product(step):
        return contract(dofs_t[:, :owned], rows_of(step, 0, owned), 1, 0)

    span = 64

    def build(step):
        for inner in range(per_step):
            group = step * per_step + inner
            start = group * lanes_of
            if not isinstance(step, int):
                start = pl.multiple_of(start, lanes_of)
            lanes = pl.ds(start, lanes_of)
            live = (lax.broadcasted_iota(jnp.int32, (1, lanes_of), 1) + start) < count
            shape = (sub, lanes_of)
            blocks = []
            patterns = []
            for slot in range(slots):
                index = index_ref[slot : slot + 1, lanes]
                if slot:
                    index = moved(index)
                weight = weight_ref[slot : slot + 1, lanes].astype(jnp.float32) * 0.125
                weight = jnp.broadcast_to(jnp.where(live, weight, 0.0), shape).astype(jnp.bfloat16)
                rest = jnp.broadcast_to(jnp.bitwise_and(index, span - 1), shape).astype(jnp.int16) - row16
                blocks.append(jnp.broadcast_to(jnp.right_shift(index, span.bit_length() - 1), shape).astype(jnp.int16))
                patterns.append(
                    [jnp.where(rest == jnp.int16(part * sub), weight, zero) for part in range(span // sub)]
                )
            summed = []
            for slot in range(slots):
                pattern = patterns[slot]
                for other in range(slot):
                    same = blocks[other] == blocks[slot]
                    pattern = [
                        mine + jnp.where(same, theirs, zero)
                        for mine, theirs in zip(pattern, patterns[other])
                    ]
                summed.append(pattern)
            for block in range(columns // span):
                values = [zero] * (span // sub)
                for slot in range(0 if block * span < owned else 1, slots):
                    match = blocks[slot] == jnp.int16(block)
                    values = [
                        jnp.where(match, mine, value)
                        for mine, value in zip(summed[slot], values)
                    ]
                for part in range(span // sub):
                    row = block * span + part * sub
                    table[group, row : row + sub, :] = values[part]

    def build_behind(step, carry):
        product = owned_product(step - 1)
        build(step)
        gathered[:, step_lanes(step - 1)] = product
        return carry

    steps = groups // per_step
    build(0)
    lax.fori_loop(1, steps, build_behind, 0)
    gathered[:, step_lanes(steps - 1)] = owned_product(steps - 1)

    def receive(chosen):
        for region in chosen:
            @pl.when(exists(me - offsets[region]))
            def _():
                ghost_copy(region).wait_recv()

    receive(order[:half])
    middle = owned + split
    dofs_t[:, owned:middle] = ghosts[:split].astype(jnp.float32).T.astype(jnp.bfloat16)

    for step in range(steps):
        gathered[:, step_lanes(step)] += contract(
            dofs_t[:, owned:middle], rows_of(step, owned, middle), 1, 0
        )
    for load in loads[5:]:
        load.wait()
    both = jnp.concatenate(
        [
            viscous_ref[...].astype(jnp.float32).T.astype(jnp.bfloat16),
            pressure_ref[...].astype(jnp.float32).T.astype(jnp.bfloat16),
        ],
        axis=0,
    )

    receive(order[half:])
    dofs_t[:, middle:] = ghosts[split:].astype(jnp.float32).T.astype(jnp.bfloat16)

    width_of = per_step
    pieces = groups // width_of

    def piece_lanes(piece):
        return pl.ds(piece * width_of * lanes_of, width_of * lanes_of)

    def upper_product(piece):
        first = piece * width_of
        rows = [table[first + inner, middle:columns, :] for inner in range(width_of)]
        return contract(dofs_t[:, middle:], jnp.concatenate(rows, axis=1), 1, 0)

    pending = [upper_product(piece) for piece in range(min(1, pieces))]
    for piece in range(pieces):
        if piece + 1 < pieces:
            pending.append(upper_product(piece + 1))
        lanes = piece_lanes(piece)
        element_in = (gathered[:, lanes] + pending[piece]).astype(jnp.bfloat16)
        applied = contract(both, element_in, 1, 0)
        result = applied[:width] * visc_ref[:, lanes] + applied[width:]
        element_out[lanes, :] = result.T.astype(jnp.bfloat16)

    def back_copy(region):
        pos = place_of[region]
        return pltpu.make_async_remote_copy(
            src_ref=back_out.at[pl.ds(pos * ghost_rows, ghost_rows)],
            dst_ref=back_in.at[pl.ds(pos * pad_rows, ghost_rows)],
            send_sem=back_send_sem.at[region],
            recv_sem=back_recv_sem.at[region],
            device_id=place(me - offsets[region]),
            device_id_type=MESH,
        )

    def scatter(low, high):
        rows = jnp.concatenate([table[group, low:high, :] for group in range(groups)], axis=1)
        return contract(rows, element_out[...], 1, 0)

    for region in upper[::-1]:
        start = place_of[region] * ghost_rows
        stop = start + ghost_rows
        back_out[start:stop] = scatter(owned + start, owned + stop).astype(jnp.bfloat16)

        @pl.when(exists(me - offsets[region]))
        def _():
            back_copy(region).start()

    late = jnp.int32(0)
    for region in upper:
        late = late + relayed(region).astype(jnp.int32)

    @pl.when(late > 0)
    def _():
        pl.semaphore_wait(late_sem, late)
    for region in order[:half]:
        start = place_of[region] * ghost_rows
        stop = start + ghost_rows
        back_out[start:stop] = scatter(owned + start, owned + stop).astype(jnp.bfloat16)

        @pl.when(exists(me - offsets[region]))
        def _():
            back_copy(region).start()

    @pl.when(any_cross(me + hop))
    def _():
        pl.semaphore_wait(ready_sem, 1)

    for region in upper:
        @pl.when(crosses(me + hop, -offsets[region]))
        def _():
            relay_copy(region).wait_recv()
            forward_copy(region).start()

    for start in range(0, owned, PIECE):
        stop = min(start + PIECE, owned)
        out_ref[start:stop] = scatter(start, stop)

    for chosen, low in ((order[:half], 0), (order[half:], half * pad_rows)):
        for region in chosen:
            @pl.when(exists(me + offsets[region]))
            def _():
                back_copy(region).wait_recv()

        high = low + half * pad_rows
        for start in range(0, owned, PIECE):
            stop = min(start + PIECE, owned)
            out_ref[start:stop] += contract(
                mirror_table[start:stop, low:high], back_in[low:high], 1, 0
            )

    for region in range(regions):
        @pl.when(direct(region))
        def _():
            ghost_copy(region).wait_send()

        if region in upper:
            @pl.when(relayed(region))
            def _():
                relay_copy(region).wait_send()

            @pl.when(crosses(me + hop, -offsets[region]))
            def _():
                forward_copy(region).wait_send()

        @pl.when(exists(me - offsets[region]))
        def _():
            back_copy(region).wait_send()


def per_device(
    n_curve,
    n_seg,
    solution,
    viscosity,
    slot_index,
    slot_weight,
    mirror_rows,
    ghost_live,
    cell_count,
    viscous_block,
    pressure_block,
):
    owned, width = solution.shape
    elems, slots = slot_index.shape
    regions, ghost_rows = mirror_rows.shape[1:]
    pad_rows = -(-ghost_rows // LANES) * LANES
    columns = owned + regions * ghost_rows
    bf16 = jnp.bfloat16
    i32 = jnp.int32
    f32 = jnp.float32
    return pl.pallas_call(
        functools.partial(operator_kernel, n_curve, n_seg),
        out_shape=jax.ShapeDtypeStruct((owned, width), jnp.float32),
        in_specs=[pl.BlockSpec(memory_space=pltpu.SMEM)]
        + [pl.BlockSpec(memory_space=pltpu.HBM)] * 8,
        out_specs=pl.BlockSpec(memory_space=pltpu.VMEM),
        scratch_shapes=[
            pltpu.VMEM((owned, width), bf16),
            pltpu.VMEM((1, elems), f32),
            pltpu.VMEM((slots, elems), i32),
            pltpu.VMEM((slots, elems), i32),
            pltpu.VMEM((regions, ghost_rows), i32),
            pltpu.VMEM((1, regions), i32),
            pltpu.VMEM((width, width), bf16),
            pltpu.VMEM((width, width), bf16),
            pltpu.VMEM((elems // LANES, columns, LANES), bf16),
            pltpu.VMEM((owned, regions * pad_rows), bf16),
            pltpu.VMEM((width, columns), bf16),
            pltpu.VMEM((width, elems), f32),
            pltpu.VMEM((elems, width), bf16),
            pltpu.VMEM((regions * pad_rows, width), bf16),
            pltpu.VMEM((regions * ghost_rows, width), bf16),
            pltpu.VMEM((regions // 2 * ghost_rows, width), bf16),
            pltpu.VMEM((regions * ghost_rows, width), bf16),
            pltpu.VMEM((regions * pad_rows, width), bf16),
            pltpu.SemaphoreType.REGULAR,
            pltpu.SemaphoreType.REGULAR,
            pltpu.SemaphoreType.DMA((regions,)),
            pltpu.SemaphoreType.DMA((regions,)),
            pltpu.SemaphoreType.DMA((regions,)),
            pltpu.SemaphoreType.DMA((8,)),
            pltpu.SemaphoreType.DMA((regions,)),
            pltpu.SemaphoreType.DMA((regions,)),
            pltpu.SemaphoreType.DMA((regions,)),
            pltpu.SemaphoreType.DMA((regions,)),
        ],
        compiler_params=pltpu.CompilerParams(
            collective_id=0, has_side_effects=True, vmem_limit_bytes=48 * 1024 * 1024
        ),
    )(
        cell_count,
        *(
            pltpu.with_memory_space_constraint(operand, pltpu.HBM)
            for operand in (
                solution,
                viscosity.reshape(1, elems),
                slot_index.T,
                slot_weight.T,
                mirror_rows.reshape(regions, ghost_rows),
                ghost_live,
                viscous_block,
                pressure_block,
            )
        )
    )


def solution(mesh):
    return jax.shard_map(
        functools.partial(per_device, mesh.shape["curve"], mesh.shape["seg"]),
        mesh=mesh,
        in_specs=(
            P(("curve", "seg"), None),
            P(("curve", "seg")),
            P(("curve", "seg"), None),
            P(("curve", "seg"), None),
            P(("curve", "seg"), None, None),
            P(("curve", "seg"), None),
            P(("curve", "seg")),
            P(),
            P(),
        ),
        out_specs=P(("curve", "seg"), None),
        check_vma=False,
    )
```
